256 devices in a mesh: band: 16 (over x_lo, z), slab: 16 (over y, x_hi, core).
Axes of the slice: x: 4 (x_hi: 2, x_lo: 2; x = x_hi * 2 + x_lo), y: 4, z: 8, core: 2. Of those that a mesh axis runs over, the one named last changes fastest.
Arguments:
- orbitals: float32 [256, 48, 2304], P('band', 'slab'), may hold values from -6 to 6
- partners: int32 [16, 2], replicated, may hold values from 0 to 15, as said below
- counts: int32 [16, 2], replicated, may hold values from 1 to 16
Outputs:
- forces: float32 [256, 48, 2304], P('band', 'slab')
- energy: float32 [], replicated
The draws below stay inside these ranges and needn't reach their ends.
Inputs may be any that keep to these rules, and one draw needn't show every extreme that they name: `partners`: row g names two different band groups, neither of them g.
All inputs are finite; a program needn't handle non-finite values.
Results may differ from the reference program's by a relative error of at most 0.0001.
Values sent between devices are 32-bit elements; how exact they have to be, the bound alone decides.
A program may use at most 64 MiB of HBM per device.

```python
import jax
import jax.numpy as jnp
from jax import lax

NX = 48
NY = 48
NZ = 48
NZP = 96
YZ = 2304
ORB_G = 16
ORBS = 256
N_BAND = 16


def draw_partners(key, part):
    first_key, second_key = jax.random.split(jax.random.fold_in(key, 17))
    groups = jnp.arange(N_BAND, dtype=jnp.int32)
    offset_one = jax.random.randint(first_key, (N_BAND,), 1, N_BAND)
    offset_two = jax.random.randint(second_key, (N_BAND,), 1, N_BAND - 1)
    offset_two = jnp.where(offset_two >= offset_one, offset_two + 1, offset_two)
    pairs = jnp.stack([(groups + offset_one) % N_BAND, (groups + offset_two) % N_BAND], axis=1)
    return pairs.astype(jnp.int32)


def with_ends(drawn, stream_key, least, largest):
    longest = drawn.shape.index(max(drawn.shape))
    spots = []
    for shift in (0, 1):
        where = [jax.random.randint(jax.random.fold_in(stream_key, axis), (), 0, length) for axis, length in enumerate(drawn.shape)]
        where[longest] = (where[longest] + shift) % drawn.shape[longest]
        spots.append(tuple(where))
    return drawn.at[spots[0]].set(least).at[spots[1]].set(largest)


def steps_of(key, shape, shards, smallest, high):
    level = 1.0
    for position, blocks in shards:
        draws = jax.random.uniform(jax.random.fold_in(jax.random.fold_in(key, 6), position), (blocks,), jnp.float32, smallest / len(shards), high / len(shards))
        level = level * jnp.repeat(jnp.exp(draws), shape[position] // blocks).reshape((-1,) + (1,) * (len(shape) - 1 - position))
    return level


def normal_values(rng, extent, spread, bound, shards=(), held_as=jnp.bfloat16):
    loudness = steps_of(rng, extent, shards, -0.22, 0.18) if shards else 1.0
    entries = jax.random.normal(rng, extent, jnp.float32) * spread * loudness
    return jnp.minimum(jnp.maximum(entries, -bound), bound).astype(held_as)


def setup_inputs(seed: int = 0) -> dict:
    seeds = jax.random.split(jax.random.key(seed), 4)
    return {
        "orbitals": normal_values(seeds[0], (ORBS, NX, YZ), 1.0, 6.0, ((0, 16), (1, 16)), jnp.float32),
        "partners": draw_partners(jax.random.fold_in(seeds[3], 71), 0),
        "counts": with_ends(jax.random.randint(seeds[2], (N_BAND, 2), 1, ORB_G + 1), jax.random.fold_in(seeds[2], 1), 1, ORB_G).astype(jnp.int32),
    }


slater_coeff = -(3.0 / 3.141592653589793) ** (1.0 / 3.0)
exchange_mix = 0.25
screening = 0.25


def kernel_grid():
    wave_x = 2.0 * jnp.pi * jnp.fft.fftfreq(NX)
    wave_y = 2.0 * jnp.pi * jnp.fft.fftfreq(NY)
    wave_z = 2.0 * jnp.pi * jnp.fft.fftfreq(NZP)
    total = wave_x[:, None, None] ** 2 + wave_y[None, :, None] ** 2 + wave_z[None, None, :] ** 2
    return 4.0 * jnp.pi / (total + screening * screening)


def screened_potential(pair_density, kernel_table):
    padded = jnp.pad(pair_density, ((0, 0), (0, 0), (0, 0), (0, NZP - NZ)))
    spectrum = jnp.fft.fftn(padded, axes=(1, 2, 3))
    potential = jnp.real(jnp.fft.ifftn(spectrum * kernel_table, axes=(1, 2, 3)))
    return potential[:, :, :, :NZ].astype(pair_density.dtype)


def reference(orbitals, partners, counts):
    orbital_grid = orbitals.reshape(N_BAND, ORB_G, NX, NY, NZ)
    density = (2.0 / ORBS) * jnp.sum(orbitals * orbitals, axis=0)
    local_pot = slater_coeff * jnp.cbrt(density)
    kernel_table = kernel_grid()
    local_rows = jnp.arange(ORB_G, dtype=jnp.int32)

    def visit(visit_step, loop_state):
        exch, energy = loop_state
        band_index = visit_step // 2
        slot_index = visit_step % 2
        partner = partners[band_index, slot_index]
        own_orbs = orbital_grid[band_index]
        partner_orbs = orbital_grid[partner]
        active = (local_rows < counts[band_index, slot_index]).astype(orbitals.dtype)
        pair_density = own_orbs * partner_orbs * active[:, None, None, None]
        pair_pot = screened_potential(pair_density, kernel_table)
        exch = exch.at[band_index].add(-exchange_mix * pair_pot * partner_orbs)
        exch = exch.at[partner].add(-exchange_mix * pair_pot * own_orbs)
        energy = energy + jnp.sum(pair_density * pair_pot)
        return exch, energy

    start = (jnp.zeros(orbital_grid.shape, jnp.float32), jnp.zeros((), jnp.float32))
    exch, energy = lax.fori_loop(0, 2 * N_BAND, visit, start)
    forces = local_pot[None] * orbitals + exch.reshape(ORBS, NX, NY * NZ)
    energy = -energy / (2.0 * ORBS * NX * NY * NZ)
    return forces, energy
```

```python
import functools
import math

import jax
import jax.numpy as jnp
import numpy as np
from jax import lax
from jax.experimental import pallas as pl
from jax.experimental.pallas import tpu as pltpu
from jax.sharding import PartitionSpec as P

NX = 48
NY = 48
NZ = 48
NZP = 96
N = 16
ROWS = 54
BLK = 56
LANES = 128
PAIRS = 2 * N
SLATER = -((3.0 / math.pi) ** (1.0 / 3.0))
MIX = 0.25
SCREENING = 0.25
F32 = jnp.float32
BF16 = jnp.bfloat16
MESH = pl.DeviceIdType.MESH


def split_np(w):
    hi = w.astype(np.float32).astype(jnp.bfloat16)
    lo = (w - hi.astype(np.float64)).astype(np.float32).astype(jnp.bfloat16)
    return hi, lo


def cas(length):
    j = np.arange(length)
    angle = 2.0 * np.pi * ((j[:, None] * j[None, :]) % length) / length
    return (np.cos(angle) + np.sin(angle)) / np.sqrt(length)


def constants():
    h = cas(48)
    order = np.array([3 * p + plane for plane in range(3) for p in range(16)])
    wx = h[:, order]

    def left(w):
        hi, lo = split_np(w)
        return np.concatenate([hi, hi, lo], axis=1)

    small = np.stack([left(wx), left(h), left(wx.T)])
    hz = cas(NZP)[:NZ, :]
    full = np.zeros((384, 8, LANES))
    for y8 in range(8):
        full[y8 * 48 : (y8 + 1) * 48, y8, :NZP] = hz
    full = full.reshape(384, 8 * LANES)
    fwd = np.concatenate(
        [full[0:128, 0:256], full[0:256, 256:512], full[128:384, 512:768], full[256:384, 768:1024]]
    )
    back = full.T
    inv01 = back[0 : 6 * 128, 0:256]
    inv2 = back[5 * 128 : 8 * 128, 256:384]
    return small, np.concatenate(split_np(fwd)), np.concatenate(split_np(inv01)), np.concatenate(split_np(inv2))


def split(x):
    hi = x.astype(BF16)
    lo = (x - hi.astype(F32)).astype(BF16)
    return hi, lo


def dot(a, b):
    return jnp.dot(a, b, preferred_element_type=F32)


def dot3(x_hl, w_hi, w_lo, m):
    both = dot(x_hl, w_hi)
    return both[:m] + both[m:] + dot(x_hl[:m], w_lo)


def left3(w3, x):
    hi, lo = split(x)
    return dot(w3, jnp.concatenate([hi, lo, hi], axis=0))


def fill_table(table):
    def wave_sq(index, length):
        signed = jnp.where(index > length // 2, index - length, index).astype(F32)
        wave = 2.0 * math.pi / length * signed
        return wave * wave

    lane = lax.broadcasted_iota(jnp.int32, (48, LANES), 1)
    row = lax.broadcasted_iota(jnp.int32, (48, LANES), 0)
    yz = wave_sq(row, NY) + wave_sq(lane, NZP) + SCREENING * SCREENING

    def step(qx, carry):
        wx = wave_sq(jnp.full((48, LANES), qx, jnp.int32), NX)
        value = jnp.where(lane < NZP, 4.0 * math.pi / (yz + wx), 0.0)
        table[pl.ds(pl.multiple_of(qx * 48, 8), 48), :] = value
        return carry

    lax.fori_loop(0, 48, step, 0)


def convolve(pd, pot, base, work, table, small, fwd, inv01, inv2):
    rows = 288

    def gather(ref, t):
        tiles = [
            ref[pl.ds(base + plane * 18 + yg * 3 + t, 16, stride=BLK), :]
            for yg in range(6)
            for plane in range(3)
        ]
        return jnp.concatenate(tiles, axis=0)

    def scatter_z(j, value):
        for yg in range(6):
            for half in range(2):
                y = yg * 8 + 2 * j + half
                work[pl.ds(y * 48, 48), :] = value[
                    yg * 48 : (yg + 1) * 48, half * LANES : (half + 1) * LANES
                ]

    def stack(t):
        hi, lo = split(gather(pd, t))
        return jnp.concatenate([hi, lo], axis=0)

    s0 = stack(0)
    scatter_z(0, dot3(s0, fwd[0:128], fwd[768 : 768 + 128], rows))
    s1 = stack(1)
    s01 = jnp.concatenate([s0, s1], axis=1)
    scatter_z(1, dot3(s01, fwd[128:384], fwd[768 + 128 : 768 + 384], rows))
    s2 = stack(2)
    s12 = jnp.concatenate([s1, s2], axis=1)
    scatter_z(2, dot3(s12, fwd[384:640], fwd[768 + 384 : 768 + 640], rows))
    scatter_z(3, dot3(s2, fwd[640:768], fwd[768 + 640 : 768 + 768], rows))

    def along_x(which):
        w3 = small[which]

        def step(i, carry):
            start = pl.multiple_of(i * 384, 8)
            block = work[pl.ds(start, 384), :]
            wide = jnp.concatenate([block[48 * u : 48 * (u + 1)] for u in range(8)], axis=1)
            out = left3(w3, wide)
            work[pl.ds(start, 384), :] = jnp.concatenate(
                [out[:, LANES * u : LANES * (u + 1)] for u in range(8)], axis=0
            )
            return carry

        lax.fori_loop(0, 6, step, 0)

    along_x(0)
    wy3 = small[1]

    def y_step(i, carry):
        qx = i * 8
        wide = jnp.concatenate(
            [work[pl.ds(qx + u, 48, stride=48), :] for u in range(8)], axis=1
        )
        spectrum = left3(wy3, wide)
        k = table[pl.ds(pl.multiple_of(qx * 48, 8), 384), :]
        k = jnp.concatenate([k[48 * u : 48 * (u + 1)] for u in range(8)], axis=1)
        out = left3(wy3, spectrum * k)
        for u in range(8):
            work[pl.ds(qx + u, 48, stride=48), :] = out[:, LANES * u : LANES * (u + 1)]
        return carry

    lax.fori_loop(0, 6, y_step, 0)
    along_x(2)

    def gather_y8(y8):
        tiles = [work[pl.ds((yg * 8 + y8) * 48, 48), :] for yg in range(6)]
        hi, lo = split(jnp.concatenate(tiles, axis=0))
        return jnp.concatenate([hi, lo], axis=0)

    energy = jnp.zeros((16, LANES), F32)

    def scatter_t(t, value, energy):
        for yg in range(6):
            for plane in range(3):
                at = pl.ds(base + plane * 18 + yg * 3 + t, 16, stride=BLK)
                tile = value[(yg * 3 + plane) * 16 : (yg * 3 + plane + 1) * 16]
                pot[at, :] = tile
                energy = energy + tile * pd[at, :]
        return energy

    parts = [gather_y8(y8) for y8 in range(6)]
    first = jnp.concatenate(parts, axis=1)
    out = dot3(first, inv01[0:768], inv01[768:1536], rows)
    energy = scatter_t(0, out[:, 0:128], energy)
    energy = scatter_t(1, out[:, 128:256], energy)
    second = jnp.concatenate([parts[5], gather_y8(6), gather_y8(7)], axis=1)
    energy = scatter_t(2, dot3(second, inv2[0:384], inv2[384:768], rows), energy)
    total = jnp.sum(energy, axis=0, keepdims=True)
    pot[pl.ds(base + ROWS, 16, stride=BLK), :] = jnp.broadcast_to(total, (16, LANES))


def block(index):
    return pl.ds(pl.multiple_of(index * BLK, 8), BLK)


def slot(ref, index):
    return ref.at[index] if len(ref.shape) == 3 else ref.at[block(index)]


def kernel(
    orb, partners, counts, small, fwd_hbm, inv01_hbm, inv2_hbm,
    forces, energy_out,
    src, held, pairs, tasks, pots, back, partial, final, ret, dens, dens_in, local, work, table, fwd, inv01, inv2,
    const_sems, sa, ra, sb, rb, sc, rc, sd, rd, sn, rn,
):
    band = lax.axis_index("band")
    slab = lax.axis_index("slab")

    def peer(me, i):
        return lax.rem(me + i, N)

    def each_peer(fn):
        def step(i, carry):
            fn(i)
            return carry

        lax.fori_loop(1, N, step, 0)

    barrier = pltpu.get_barrier_semaphore()

    def greet(i):
        pl.semaphore_signal(barrier, inc=1, device_id={"band": peer(band, i)}, device_id_type=MESH)
        pl.semaphore_signal(barrier, inc=1, device_id={"slab": peer(slab, i)}, device_id_type=MESH)

    each_peer(greet)
    loads = [
        pltpu.make_async_copy(a, b, const_sems.at[i])
        for i, (a, b) in enumerate(((fwd_hbm, fwd), (inv01_hbm, inv01), (inv2_hbm, inv2)))
    ]
    for load in loads:
        load.start()

    for plane in range(3):
        for chunk in range(18):
            tile = orb[plane, :, chunk * LANES : (chunk + 1) * LANES]
            src[pl.ds(plane * 18 + chunk, N, stride=BLK), :] = tile
            dens[pl.ds(plane * 18 + chunk, 1), :] = jnp.sum(tile * tile, axis=0, keepdims=True)
    pl.semaphore_wait(barrier, 2 * (N - 1))

    def band_copy(a, b, at_peer, at_me, send, recv, i):
        p = peer(band, i)
        return pltpu.make_async_remote_copy(
            src_ref=a.at[block(p)] if at_peer else a,
            dst_ref=slot(b, at_me),
            send_sem=send.at[p],
            recv_sem=recv.at[at_me],
            device_id={"band": p},
            device_id_type=MESH,
        )

    def slab_copy(a, b, k, send, recv, i):
        p = peer(slab, i)
        return pltpu.make_async_remote_copy(
            src_ref=a.at[block(k * N + p)],
            dst_ref=b.at[block(k * N + slab)],
            send_sem=send.at[k * N + p],
            recv_sem=recv.at[k * N + slab],
            device_id={"slab": p},
            device_id_type=MESH,
        )

    def landed(b, k, at, recv, send, p):
        return pltpu.make_async_remote_copy(
            src_ref=slot(b, k * N + p),
            dst_ref=slot(b, k * N + p),
            send_sem=send.at[k * N + p],
            recv_sem=recv.at[k * N + p],
            device_id=at,
            device_id_type=MESH,
        )

    def wait_band(b, recv, send):
        each_peer(
            lambda i: landed(b, 0, {"band": peer(band, i)}, recv, send, peer(band, i)).wait_recv()
        )

    def wait_slab(b, k, recv, send):
        each_peer(
            lambda i: landed(b, k, {"slab": peer(slab, i)}, recv, send, peer(slab, i)).wait_recv()
        )

    each_peer(lambda i: band_copy(src, held, True, band, sa, ra, i).start())
    held[band] = src[block(band), :]
    each_peer(lambda i: band_copy(dens, dens_in, False, band, sn, rn, i).start())
    dens_in[block(band), :] = dens[...]

    fill_table(table)
    wait_band(held, ra, sa)

    for k in range(2):
        def pair(g, k=k):
            partner = partners[k, g]
            active = jnp.where(band < counts[k, g], 1.0, 0.0).astype(F32)
            return held[g] * held[partner] * active

        def send_pair(i, k=k):
            g = peer(slab, i)
            pairs[block(k * N + g), :] = pair(g)
            slab_copy(pairs, tasks, k, sb, rb, i).start()

        each_peer(send_pair)
        tasks[block(k * N + slab), :] = pair(slab)

    for load in loads:
        load.wait()

    for k in range(2):
        wait_slab(tasks, k, rb, sb)
        convolve(tasks, pots, k * N * BLK, work, table, small, fwd, inv01, inv2)
        each_peer(lambda i: slab_copy(pots, back, k, sc, rc, i).start())
        back[block(k * N + slab), :] = pots[block(k * N + slab), :]

    wait_band(dens_in, rn, sn)
    total = dens_in[pl.ds(0, BLK), :]
    for b in range(1, N):
        total = total + dens_in[pl.ds(b * BLK, BLK), :]
    total = total * (2.0 / (N * N))
    safe = jnp.maximum(total, 1e-37)
    root = jnp.exp(jnp.log(safe) * (1.0 / 3.0))
    root = root * (2.0 + safe / (root * root * root)) * (1.0 / 3.0)
    local[...] = SLATER * jnp.where(total > 0.0, root, 0.0)

    row = lax.broadcasted_iota(jnp.int32, (N, PAIRS), 0)
    col = lax.broadcasted_iota(jnp.int32, (N, PAIRS), 1)
    names = jnp.full((N, PAIRS), -1, jnp.int32)
    for k in range(2):
        for g in range(N):
            names = jnp.where(col == k * N + g, partners[k, g], names)
    onehot = jnp.where(names == row, 1.0, 0.0).astype(BF16)
    onehot3 = jnp.concatenate([onehot, onehot, onehot], axis=1)

    wait_slab(back, 0, rc, sc)
    wait_slab(back, 1, rc, sc)

    def own_terms(g, carry):
        phi = held[g]
        own = jnp.zeros((BLK, LANES), F32)
        for k in range(2):
            pot = back[block(k * N + g), :]
            own = own + pot * held[partners[k, g]]
            ret[block(k * N + g), :] = pot * phi
        partial[block(g), :] = own
        return carry

    lax.fori_loop(0, N, own_terms, 0)

    for first in range(0, ROWS, 9):
        wide = jnp.concatenate(
            [ret[pl.ds(first + u, PAIRS, stride=BLK), :] for u in range(9)], axis=1
        )
        hi, mid = split(wide)
        low = (wide - hi.astype(F32) - mid.astype(F32)).astype(BF16)
        summed = dot(onehot3, jnp.concatenate([hi, mid, low], axis=0))
        for u in range(9):
            at = pl.ds(first + u, N, stride=BLK)
            partial[at, :] = -MIX * (partial[at, :] + summed[:, u * LANES : (u + 1) * LANES])
    index_energy = jnp.sum(back[pl.ds(ROWS, PAIRS, stride=BLK), :], axis=0, keepdims=True)
    partial[pl.ds(ROWS, N, stride=BLK), :] = jnp.broadcast_to(index_energy, (N, LANES))

    each_peer(lambda i: band_copy(partial, final, True, band, sd, rd, i).start())
    final[block(band), :] = partial[block(band), :]
    wait_band(final, rd, sd)

    for plane in range(3):
        for chunk in range(18):
            r = plane * 18 + chunk
            lanes = slice(chunk * LANES, (chunk + 1) * LANES)
            forces[plane, :, lanes] = (
                local[pl.ds(r, 1), :] * orb[plane, :, lanes] + final[pl.ds(r, N, stride=BLK), :]
            )
    energies = final[pl.ds(ROWS, N, stride=BLK), :]
    energy_out[0, 0] = jnp.sum(energies) * (-1.0 / (2.0 * N * N * NX * NY * NZ))

    each_peer(lambda i: band_copy(src, held, True, band, sa, ra, i).wait_send())
    each_peer(lambda i: band_copy(dens, dens_in, False, band, sn, rn, i).wait_send())
    for k in range(2):
        each_peer(lambda i: slab_copy(pairs, tasks, k, sb, rb, i).wait_send())
        each_peer(lambda i: slab_copy(pots, back, k, sc, rc, i).wait_send())
    each_peer(lambda i: band_copy(partial, final, True, band, sd, rd, i).wait_send())


def solution(mesh):
    small, fwd, inv01, inv2 = constants()
    vmem = pl.BlockSpec(memory_space=pltpu.VMEM)
    smem = pl.BlockSpec(memory_space=pltpu.SMEM)
    hbm = pl.BlockSpec(memory_space=pl.ANY)
    one = (N * BLK, LANES)
    two = (2 * N * BLK, LANES)
    sems = lambda n: pltpu.SemaphoreType.DMA((n,))

    def body(orbitals, partners, counts):
        forces, energy = pl.pallas_call(
            kernel,
            out_shape=(
                jax.ShapeDtypeStruct((3, N, NY * NZ), F32),
                jax.ShapeDtypeStruct((1, 1), F32),
            ),
            in_specs=[vmem, smem, smem, vmem, hbm, hbm, hbm],
            out_specs=(vmem, smem),
            scratch_shapes=[
                pltpu.VMEM(one, F32),
                pltpu.VMEM((N, BLK, LANES), F32),
                pltpu.VMEM(two, F32),
                pltpu.VMEM(two, F32),
                pltpu.VMEM(two, F32),
                pltpu.VMEM(two, F32),
                pltpu.VMEM(one, F32),
                pltpu.VMEM(one, F32),
                pltpu.VMEM(two, F32),
                pltpu.VMEM((BLK, LANES), F32),
                pltpu.VMEM(one, F32),
                pltpu.VMEM((BLK, LANES), F32),
                pltpu.VMEM((48 * 48, LANES), F32),
                pltpu.VMEM((48 * 48, LANES), F32),
                pltpu.VMEM(fwd.shape, BF16),
                pltpu.VMEM(inv01.shape, BF16),
                pltpu.VMEM(inv2.shape, BF16),
                sems(3),
                sems(N), sems(N),
                sems(2 * N), sems(2 * N),
                sems(2 * N), sems(2 * N),
                sems(N), sems(N),
                sems(N), sems(N),
            ],
            compiler_params=pltpu.CompilerParams(
                collective_id=0, has_side_effects=True, vmem_limit_bytes=48 * 1024 * 1024
            ),
        )(
            orbitals.transpose(1, 0, 2), partners.T, counts.T,
            jnp.asarray(small), jnp.asarray(fwd), jnp.asarray(inv01), jnp.asarray(inv2),
        )
        return forces.transpose(1, 0, 2), energy.reshape(())

    specs = P("band", "slab", None)
    return jax.shard_map(
        body, mesh=mesh, in_specs=(specs, P(), P()), out_specs=(specs, P()), check_vma=False
    )
```

```python
import functools
import math

import jax
import jax.numpy as jnp
import numpy as np
from jax import lax
from jax.experimental import pallas as pl
from jax.experimental.pallas import tpu as pltpu
from jax.sharding import PartitionSpec as P

NX = 48
NY = 48
NZ = 48
NZP = 96
N = 16
ROWS = 54
BLK = 56
LANES = 128
CHUNKS = ((0, 24), (24, 16), (40, 16))
PAIRS = 2 * N
SLATER = -((3.0 / math.pi) ** (1.0 / 3.0))
MIX = 0.25
VMEM_BYTES = 67_043_328
SCREENING = 0.25
F32 = jnp.float32
BF16 = jnp.bfloat16
MESH = pl.DeviceIdType.MESH


def split_np(w):
    hi = w.astype(np.float32).astype(jnp.bfloat16)
    lo = (w - hi.astype(np.float64)).astype(np.float32).astype(jnp.bfloat16)
    return hi, lo


def cas(length):
    j = np.arange(length)
    angle = 2.0 * np.pi * ((j[:, None] * j[None, :]) % length) / length
    return (np.cos(angle) + np.sin(angle)) / np.sqrt(length)


def constants():
    h = cas(48)
    order = np.array([3 * p + plane for plane in range(3) for p in range(16)])
    wx = h[:, order]

    def left(w):
        hi, lo = split_np(w)
        return np.concatenate([hi, hi, lo], axis=1)

    small = np.stack([left(wx), left(h), left(wx.T)])
    hz = cas(NZP)[:NZ, :]
    full = np.zeros((384, 8, LANES))
    for y8 in range(8):
        full[y8 * 48 : (y8 + 1) * 48, y8, :NZP] = hz
    full = full.reshape(384, 8 * LANES)
    fwd = np.concatenate(
        [full[0:128, 0:256], full[0:256, 256:512], full[128:384, 512:768], full[256:384, 768:1024]]
    )
    back = full.T
    inv01 = back[0 : 6 * 128, 0:256]
    inv2 = back[5 * 128 : 8 * 128, 256:384]
    return small, np.concatenate(split_np(fwd)), np.concatenate(split_np(inv01)), np.concatenate(split_np(inv2))


def split(x):
    hi = x.astype(BF16)
    lo = (x - hi.astype(F32)).astype(BF16)
    return hi, lo


def dot(a, b):
    return jnp.dot(a, b, preferred_element_type=F32)


def dot3(x_hl, w_hi, w_lo, m):
    both = dot(x_hl, w_hi)
    return both[:m] + both[m:] + dot(x_hl[:m], w_lo)


def left3(w3, x):
    hi, lo = split(x)
    return dot(w3, jnp.concatenate([hi, lo, hi], axis=0))


def fill_table(table):
    def wave_sq(index, length):
        signed = jnp.where(index > length // 2, index - length, index).astype(F32)
        wave = 2.0 * math.pi / length * signed
        return wave * wave

    lane = lax.broadcasted_iota(jnp.int32, (48, LANES), 1)
    row = lax.broadcasted_iota(jnp.int32, (48, LANES), 0)
    yz = wave_sq(row, NY) + wave_sq(lane, NZP) + SCREENING * SCREENING

    def step(qx, carry):
        wx = wave_sq(jnp.full((48, LANES), qx, jnp.int32), NX)
        value = jnp.where(lane < NZP, 4.0 * math.pi / (yz + wx), 0.0)
        table[pl.ds(pl.multiple_of(qx * 48, 8), 48), :] = value
        return carry

    lax.fori_loop(0, 48, step, 0)


def convolve(pd, pot, base, work, table, small, fwd, inv01, inv2):
    rows = 288

    def gather(ref, t):
        tiles = [
            ref[pl.ds(base + plane * 18 + yg * 3 + t, 16, stride=BLK), :]
            for yg in range(6)
            for plane in range(3)
        ]
        return jnp.concatenate(tiles, axis=0)

    def scatter_z(j, value):
        for yg in range(6):
            for half in range(2):
                y = yg * 8 + 2 * j + half
                work[pl.ds(y * 48, 48), :] = value[
                    yg * 48 : (yg + 1) * 48, half * LANES : (half + 1) * LANES
                ]

    def stack(t):
        hi, lo = split(gather(pd, t))
        return jnp.concatenate([hi, lo], axis=0)

    s0 = stack(0)
    scatter_z(0, dot3(s0, fwd[0:128], fwd[768 : 768 + 128], rows))
    s1 = stack(1)
    s01 = jnp.concatenate([s0, s1], axis=1)
    scatter_z(1, dot3(s01, fwd[128:384], fwd[768 + 128 : 768 + 384], rows))
    s2 = stack(2)
    s12 = jnp.concatenate([s1, s2], axis=1)
    scatter_z(2, dot3(s12, fwd[384:640], fwd[768 + 384 : 768 + 640], rows))
    scatter_z(3, dot3(s2, fwd[640:768], fwd[768 + 640 : 768 + 768], rows))

    def along_x(which):
        w3 = small[which]

        def step(i, carry):
            start = pl.multiple_of(i * 384, 8)
            block = work[pl.ds(start, 384), :]
            wide = jnp.concatenate([block[48 * u : 48 * (u + 1)] for u in range(8)], axis=1)
            out = left3(w3, wide)
            work[pl.ds(start, 384), :] = jnp.concatenate(
                [out[:, LANES * u : LANES * (u + 1)] for u in range(8)], axis=0
            )
            return carry

        lax.fori_loop(0, 6, step, 0)

    along_x(0)
    wy3 = small[1]

    def y_step(i, carry):
        qx = i * 8
        wide = jnp.concatenate(
            [work[pl.ds(qx + u, 48, stride=48), :] for u in range(8)], axis=1
        )
        spectrum = left3(wy3, wide)
        k = table[pl.ds(pl.multiple_of(qx * 48, 8), 384), :]
        k = jnp.concatenate([k[48 * u : 48 * (u + 1)] for u in range(8)], axis=1)
        out = left3(wy3, spectrum * k)
        for u in range(8):
            work[pl.ds(qx + u, 48, stride=48), :] = out[:, LANES * u : LANES * (u + 1)]
        return carry

    lax.fori_loop(0, 6, y_step, 0)
    along_x(2)

    def gather_y8(y8):
        tiles = [work[pl.ds((yg * 8 + y8) * 48, 48), :] for yg in range(6)]
        hi, lo = split(jnp.concatenate(tiles, axis=0))
        return jnp.concatenate([hi, lo], axis=0)

    energy = jnp.zeros((16, LANES), F32)

    def scatter_t(t, value, energy):
        for yg in range(6):
            for plane in range(3):
                at = pl.ds(base + plane * 18 + yg * 3 + t, 16, stride=BLK)
                tile = value[(yg * 3 + plane) * 16 : (yg * 3 + plane + 1) * 16]
                pot[at, :] = tile
                energy = energy + tile * pd[at, :]
        return energy

    parts = [gather_y8(y8) for y8 in range(6)]
    first = jnp.concatenate(parts, axis=1)
    out = dot3(first, inv01[0:768], inv01[768:1536], rows)
    energy = scatter_t(0, out[:, 0:128], energy)
    energy = scatter_t(1, out[:, 128:256], energy)
    second = jnp.concatenate([parts[5], gather_y8(6), gather_y8(7)], axis=1)
    energy = scatter_t(2, dot3(second, inv2[0:384], inv2[384:768], rows), energy)
    total = jnp.sum(energy, axis=0, keepdims=True)
    pot[pl.ds(base + ROWS, 16, stride=BLK), :] = jnp.broadcast_to(total, (16, LANES))


def rows_of(index, first, count):
    return pl.ds(pl.multiple_of(index * BLK + first, 8), count)


def block(index):
    return rows_of(index, 0, BLK)


def kernel(
    orb_hbm, partners_hbm, counts_hbm, small_hbm, fwd_hbm, inv01_hbm, inv2_hbm,
    forces, energy_out,
    orb, partners, counts, small, fwd, inv01, inv2,
    src, held0, held1, held2, pairs, tasks, pots, back, partial, final, ret, dens, dens_in, local, work, table,
    load_sems, sa, ra, sb, rb, sc, rc, sd, rd, sn, rn,
):
    band = lax.axis_index("band")
    slab = lax.axis_index("slab")
    held = (held0, held1, held2)

    loads = [
        pltpu.make_async_copy(a, b, load_sems.at[i])
        for i, (a, b) in enumerate(
            (
                (orb_hbm, orb), (partners_hbm, partners), (counts_hbm, counts),
                (small_hbm, small), (fwd_hbm, fwd), (inv01_hbm, inv01), (inv2_hbm, inv2),
            )
        )
    ]
    for load in loads:
        load.start()

    def peer(me, i):
        return lax.rem(me + i, N)

    def each_peer(fn):
        def step(i, carry):
            fn(i)
            return carry

        lax.fori_loop(1, N, step, 0)

    barrier = pltpu.get_barrier_semaphore()

    def greet(i):
        pl.semaphore_signal(barrier, inc=1, device_id={"band": peer(band, i)}, device_id_type=MESH)
        pl.semaphore_signal(barrier, inc=1, device_id={"slab": peer(slab, i)}, device_id_type=MESH)

    each_peer(greet)
    loads[0].wait()

    for plane in range(3):
        for chunk in range(18):
            tile = orb[plane, :, chunk * LANES : (chunk + 1) * LANES]
            src[pl.ds(plane * 18 + chunk, N, stride=BLK), :] = tile
            dens[pl.ds(plane * 18 + chunk, 1), :] = jnp.sum(tile * tile, axis=0, keepdims=True)
    pl.semaphore_wait(barrier, 2 * (N - 1))

    def remote(a, b, send, recv, axis, p):
        return pltpu.make_async_remote_copy(
            src_ref=a, dst_ref=b, send_sem=send, recv_sem=recv,
            device_id={axis: p}, device_id_type=MESH,
        )

    def orbital_copy(c, p, at):
        first, count = CHUNKS[c]
        return remote(
            src.at[rows_of(p, first, count)], held[c].at[at],
            sa.at[c * N + p], ra.at[c * N + at], "band", p,
        )

    def square_copy(p, at):
        return remote(dens, dens_in.at[block(at)], sn.at[p], rn.at[at], "band", p)

    def pair_copy(k, c, p, at):
        first, count = CHUNKS[c]
        sem = (k * 3 + c) * N
        return remote(
            pairs.at[rows_of(k * N + p, first, count)], tasks.at[rows_of(k * N + at, first, count)],
            sb.at[sem + p], rb.at[sem + at], "slab", p,
        )

    def pot_copy(k, c, p, at):
        first, count = CHUNKS[c]
        sem = (k * 3 + c) * N
        return remote(
            pots.at[rows_of(k * N + p, first, count)], back.at[rows_of(k * N + at, first, count)],
            sc.at[sem + p], rc.at[sem + at], "slab", p,
        )

    def exchange_copy(c, p, at):
        first, count = CHUNKS[c]
        return remote(
            partial.at[rows_of(p, first, count)], final.at[rows_of(at, first, count)],
            sd.at[c * N + p], rd.at[c * N + at], "band", p,
        )

    for c in range(3):
        each_peer(lambda i, c=c: orbital_copy(c, peer(band, i), band).start())
    each_peer(lambda i: square_copy(peer(band, i), band).start())
    for c, (first, count) in enumerate(CHUNKS):
        held[c][band] = src[rows_of(band, first, count), :]
    dens_in[block(band), :] = dens[...]

    fill_table(table)
    loads[1].wait()
    loads[2].wait()

    for c, (first, count) in enumerate(CHUNKS):
        each_peer(lambda i, c=c: orbital_copy(c, peer(band, i), peer(band, i)).wait_recv())
        for k in range(2):
            def pair(g, k=k, c=c):
                partner = partners[k, g]
                active = jnp.where(band < counts[k, g], 1.0, 0.0).astype(F32)
                return held[c][g] * held[c][partner] * active

            def send_pair(i, k=k, c=c, first=first, count=count, pair=pair):
                g = peer(slab, i)
                pairs[rows_of(k * N + g, first, count), :] = pair(g)
                pair_copy(k, c, g, slab).start()

            each_peer(send_pair)
            tasks[rows_of(k * N + slab, first, count), :] = pair(slab)

    for load in loads[3:]:
        load.wait()

    for k in range(2):
        for c in range(3):
            each_peer(lambda i, k=k, c=c: pair_copy(k, c, peer(slab, i), peer(slab, i)).wait_recv())
        convolve(tasks, pots, k * N * BLK, work, table, small, fwd, inv01, inv2)
        for c in range(3):
            each_peer(lambda i, k=k, c=c: pot_copy(k, c, peer(slab, i), slab).start())
        back[block(k * N + slab), :] = pots[block(k * N + slab), :]

    each_peer(lambda i: square_copy(peer(band, i), peer(band, i)).wait_recv())
    total = dens_in[pl.ds(0, BLK), :]
    for b in range(1, N):
        total = total + dens_in[pl.ds(b * BLK, BLK), :]
    total = total * (2.0 / (N * N))
    safe = jnp.maximum(total, 1e-37)
    root = jnp.exp(jnp.log(safe) * (1.0 / 3.0))
    root = root * (2.0 + safe / (root * root * root)) * (1.0 / 3.0)
    local[...] = SLATER * jnp.where(total > 0.0, root, 0.0)

    row = lax.broadcasted_iota(jnp.int32, (N, PAIRS), 0)
    col = lax.broadcasted_iota(jnp.int32, (N, PAIRS), 1)
    names = jnp.full((N, PAIRS), -1, jnp.int32)
    for k in range(2):
        for g in range(N):
            names = jnp.where(col == k * N + g, partners[k, g], names)
    onehot = jnp.where(names == row, 1.0, 0.0).astype(BF16)
    onehot3 = jnp.concatenate([onehot, onehot, onehot], axis=1)

    for c, (first, count) in enumerate(CHUNKS):
        for k in range(2):
            each_peer(lambda i, k=k, c=c: pot_copy(k, c, peer(slab, i), peer(slab, i)).wait_recv())

        def own_terms(g, carry, c=c, first=first, count=count):
            phi = held[c][g]
            own = jnp.zeros((count, LANES), F32)
            for k in range(2):
                pot = back[rows_of(k * N + g, first, count), :]
                own = own + pot * held[c][partners[k, g]]
                ret[rows_of(k * N + g, first, count), :] = pot * phi
            partial[rows_of(g, first, count), :] = own
            return carry

        lax.fori_loop(0, N, own_terms, 0, unroll=2)
        for eight in range(first, first + count, 8):
            wide = jnp.concatenate(
                [ret[pl.ds(eight + u, PAIRS, stride=BLK), :] for u in range(8)], axis=1
            )
            hi, mid = split(wide)
            low = (wide - hi.astype(F32) - mid.astype(F32)).astype(BF16)
            summed = dot(onehot3, jnp.concatenate([hi, mid, low], axis=0))
            for u in range(min(8, ROWS - eight)):
                at = pl.ds(eight + u, N, stride=BLK)
                partial[at, :] = -MIX * (partial[at, :] + summed[:, u * LANES : (u + 1) * LANES])
        if c == 2:
            index_energy = jnp.sum(back[pl.ds(ROWS, PAIRS, stride=BLK), :], axis=0, keepdims=True)
            partial[pl.ds(ROWS, N, stride=BLK), :] = jnp.broadcast_to(index_energy, (N, LANES))
        each_peer(lambda i, c=c: exchange_copy(c, peer(band, i), band).start())
        final[rows_of(band, first, count), :] = partial[rows_of(band, first, count), :]

    for c, (first, count) in enumerate(CHUNKS):
        each_peer(lambda i, c=c: exchange_copy(c, peer(band, i), peer(band, i)).wait_recv())
        for r in range(first, min(ROWS, first + count)):
            plane, chunk = divmod(r, 18)
            lanes = slice(chunk * LANES, (chunk + 1) * LANES)
            forces[plane, :, lanes] = (
                local[pl.ds(r, 1), :] * orb[plane, :, lanes] + final[pl.ds(r, N, stride=BLK), :]
            )
    energies = final[pl.ds(ROWS, N, stride=BLK), :]
    energy_out[0, 0] = jnp.sum(energies) * (-1.0 / (2.0 * N * N * NX * NY * NZ))

    each_peer(lambda i: square_copy(peer(band, i), band).wait_send())
    for c in range(3):
        each_peer(lambda i, c=c: orbital_copy(c, peer(band, i), band).wait_send())
        each_peer(lambda i, c=c: exchange_copy(c, peer(band, i), band).wait_send())
        for k in range(2):
            each_peer(lambda i, k=k, c=c: pair_copy(k, c, peer(slab, i), slab).wait_send())
            each_peer(lambda i, k=k, c=c: pot_copy(k, c, peer(slab, i), slab).wait_send())


def solution(mesh):
    small, fwd, inv01, inv2 = constants()
    vmem = pl.BlockSpec(memory_space=pltpu.VMEM)
    smem = pl.BlockSpec(memory_space=pltpu.SMEM)
    hbm = pl.BlockSpec(memory_space=pl.ANY)
    one = pltpu.VMEM((N * BLK, LANES), F32)
    two = pltpu.VMEM((2 * N * BLK, LANES), F32)
    line = pltpu.VMEM((BLK, LANES), F32)
    grid = pltpu.VMEM((48 * 48, LANES), F32)
    sems = lambda n: pltpu.SemaphoreType.DMA((n,))

    def body(orbitals, partners, counts):
        forces, energy = pl.pallas_call(
            kernel,
            out_shape=(
                jax.ShapeDtypeStruct((3, N, NY * NZ), F32),
                jax.ShapeDtypeStruct((1, 1), F32),
            ),
            in_specs=[hbm] * 7,
            out_specs=(vmem, smem),
            scratch_shapes=[
                pltpu.VMEM((3, N, NY * NZ), F32),
                pltpu.SMEM((2, N), jnp.int32),
                pltpu.SMEM((2, N), jnp.int32),
                *[pltpu.VMEM(w.shape, BF16) for w in (small, fwd, inv01, inv2)],
                one,
                *[pltpu.VMEM((N, count, LANES), F32) for _, count in CHUNKS],
                two, two, two, two,
                one, one,
                two,
                line, one, line,
                grid, grid,
                sems(7),
                sems(3 * N), sems(3 * N),
                sems(6 * N), sems(6 * N),
                sems(6 * N), sems(6 * N),
                sems(3 * N), sems(3 * N),
                sems(N), sems(N),
            ],
            compiler_params=pltpu.CompilerParams(
                collective_id=0, has_side_effects=True, vmem_limit_bytes=VMEM_BYTES
            ),
        )(
            orbitals.transpose(1, 0, 2), partners.T, counts.T,
            jnp.asarray(small), jnp.asarray(fwd), jnp.asarray(inv01), jnp.asarray(inv2),
        )
        return forces.transpose(1, 0, 2), energy.reshape(())

    specs = P("band", "slab", None)
    return jax.shard_map(
        body, mesh=mesh, in_specs=(specs, P(), P()), out_specs=(specs, P()), check_vma=False
    )
```

```python
import functools
import math

import jax
import jax.numpy as jnp
import numpy as np
from jax import lax
from jax.experimental import pallas as pl
from jax.experimental.pallas import tpu as pltpu
from jax.sharding import PartitionSpec as P

NX = 48
NY = 48
NZ = 48
NZP = 96
N = 16
ROWS = 54
BLK = 56
LANES = 128
CHUNKS = ((0, BLK),)
PARTS = len(CHUNKS)
TILES = BLK // 8
PAIRS = 2 * N
SLATER = -((3.0 / math.pi) ** (1.0 / 3.0))
MIX = 0.25
VMEM_BYTES = 65_600_000
SCREENING = 0.25
F32 = jnp.float32
BF16 = jnp.bfloat16
MESH = pl.DeviceIdType.MESH


def split_np(w):
    hi = w.astype(np.float32).astype(jnp.bfloat16)
    lo = (w - hi.astype(np.float64)).astype(np.float32).astype(jnp.bfloat16)
    return hi, lo


def cas(length):
    j = np.arange(length)
    angle = 2.0 * np.pi * ((j[:, None] * j[None, :]) % length) / length
    return (np.cos(angle) + np.sin(angle)) / np.sqrt(length)


def constants():
    h = cas(48)
    order = np.array([3 * p + plane for plane in range(3) for p in range(16)])
    wx = h[:, order]

    def left(w):
        hi, lo = split_np(w)
        return np.concatenate([hi, hi, lo], axis=1)

    small = np.stack([left(wx), left(h), left(wx.T)])
    hz = cas(NZP)[:NZ, :]
    full = np.zeros((384, 8, LANES))
    for y8 in range(8):
        full[y8 * 48 : (y8 + 1) * 48, y8, :NZP] = hz
    full = full.reshape(384, 8 * LANES)
    fwd = np.concatenate(
        [full[0:128, 0:256], full[0:256, 256:512], full[128:384, 512:768], full[256:384, 768:1024]]
    )
    back = full.T
    inv01 = back[0 : 6 * 128, 0:256]
    inv2 = back[5 * 128 : 8 * 128, 256:384]
    small = np.pad(small.reshape(144, 144), ((0, 0), (0, 112)))
    return np.concatenate(
        [*split_np(fwd), *split_np(inv01), np.concatenate(split_np(inv2), axis=1), small]
    )


def split(x):
    hi = x.astype(BF16)
    lo = (x - hi.astype(F32)).astype(BF16)
    return hi, lo


def dot(a, b):
    return jnp.dot(a, b, preferred_element_type=F32)


def dot3(x_hl, w_hi, w_lo, m):
    both = dot(x_hl, w_hi)
    return both[:m] + both[m:] + dot(x_hl[:m], w_lo)


def left3(w3, x):
    hi, lo = split(x)
    return dot(w3, jnp.concatenate([hi, lo, hi], axis=0))


def fill_table(table):
    def wave_sq(index, length):
        signed = jnp.where(index > length // 2, index - length, index).astype(F32)
        wave = 2.0 * math.pi / length * signed
        return wave * wave

    lane = lax.broadcasted_iota(jnp.int32, (48, LANES), 1)
    row = lax.broadcasted_iota(jnp.int32, (48, LANES), 0)
    yz = wave_sq(row, NY) + wave_sq(lane, NZP) + SCREENING * SCREENING

    def step(qx, carry):
        wx = wave_sq(jnp.full((48, LANES), qx, jnp.int32), NX)
        value = jnp.where(lane < NZP, 4.0 * math.pi / (yz + wx), 0.0)
        table[pl.ds(pl.multiple_of(qx * 48, 8), 48), :] = value
        return carry

    lax.fori_loop(0, 48, step, 0)


def convolve(pd, pot, base, work, table, dft):
    rows = 288

    def gather(ref, t):
        tiles = [
            ref[pl.ds(base + plane * 18 + yg * 3 + t, 16, stride=BLK), :]
            for yg in range(6)
            for plane in range(3)
        ]
        return jnp.concatenate(tiles, axis=0)

    def scatter_z(j, value):
        for yg in range(6):
            for half in range(2):
                y = yg * 8 + 2 * j + half
                work[pl.ds(y * 48, 48), :] = value[
                    yg * 48 : (yg + 1) * 48, half * LANES : (half + 1) * LANES
                ]

    def stack(t):
        hi, lo = split(gather(pd, t))
        return jnp.concatenate([hi, lo], axis=0)

    s0 = stack(0)
    scatter_z(0, dot3(s0, dft[0:128], dft[768 : 768 + 128], rows))
    s1 = stack(1)
    s01 = jnp.concatenate([s0, s1], axis=1)
    scatter_z(1, dot3(s01, dft[128:384], dft[768 + 128 : 768 + 384], rows))
    s2 = stack(2)
    s12 = jnp.concatenate([s1, s2], axis=1)
    scatter_z(2, dot3(s12, dft[384:640], dft[768 + 384 : 768 + 640], rows))
    scatter_z(3, dot3(s2, dft[640:768], dft[768 + 640 : 768 + 768], rows))

    def along_x(which):
        w3 = dft[3456 + 48 * which : 3504 + 48 * which, 0:144]

        def step(i, carry):
            start = pl.multiple_of(i * 384, 8)
            block = work[pl.ds(start, 384), :]
            wide = jnp.concatenate([block[48 * u : 48 * (u + 1)] for u in range(8)], axis=1)
            out = left3(w3, wide)
            work[pl.ds(start, 384), :] = jnp.concatenate(
                [out[:, LANES * u : LANES * (u + 1)] for u in range(8)], axis=0
            )
            return carry

        lax.fori_loop(0, 6, step, 0, unroll=6)

    along_x(0)
    wy3 = dft[3504:3552, 0:144]

    def y_step(i, carry):
        qx = i * 8
        wide = jnp.concatenate(
            [work[pl.ds(qx + u, 48, stride=48), :] for u in range(8)], axis=1
        )
        spectrum = left3(wy3, wide)
        k = table[pl.ds(pl.multiple_of(qx * 48, 8), 384), :]
        k = jnp.concatenate([k[48 * u : 48 * (u + 1)] for u in range(8)], axis=1)
        out = left3(wy3, spectrum * k)
        for u in range(8):
            work[pl.ds(qx + u, 48, stride=48), :] = out[:, LANES * u : LANES * (u + 1)]
        return carry

    lax.fori_loop(0, 6, y_step, 0, unroll=6)
    along_x(2)

    def gather_y8(y8):
        tiles = [work[pl.ds((yg * 8 + y8) * 48, 48), :] for yg in range(6)]
        hi, lo = split(jnp.concatenate(tiles, axis=0))
        return jnp.concatenate([hi, lo], axis=0)

    energy = jnp.zeros((16, LANES), F32)

    def scatter_t(t, value, energy):
        for yg in range(6):
            for plane in range(3):
                at = pl.ds(base + plane * 18 + yg * 3 + t, 16, stride=BLK)
                tile = value[(yg * 3 + plane) * 16 : (yg * 3 + plane + 1) * 16]
                pot[at, :] = tile
                energy = energy + tile * pd[at, :]
        return energy

    parts = [gather_y8(y8) for y8 in range(6)]
    first = jnp.concatenate(parts, axis=1)
    out = dot3(first, dft[1536:2304], dft[2304:3072], rows)
    energy = scatter_t(0, out[:, 0:128], energy)
    energy = scatter_t(1, out[:, 128:256], energy)
    second = jnp.concatenate([parts[5], gather_y8(6), gather_y8(7)], axis=1)
    energy = scatter_t(2, dot3(second, dft[3072:3456, 0:128], dft[3072:3456, 128:256], rows), energy)
    total = jnp.sum(energy, axis=0, keepdims=True)
    pot[pl.ds(base + ROWS, 16, stride=BLK), :] = jnp.broadcast_to(total, (16, LANES))


def rows_of(index, first, count):
    return pl.ds(pl.multiple_of(index * BLK + first, 8), count)


def block(index):
    return rows_of(index, 0, BLK)


def kernel(
    orb_hbm, partners_hbm, counts_hbm, dft_hbm,
    forces, energy_out,
    orb, partners, counts, dft,
    src, pairs, tasks, pots, back, partial, final, ret, dens, dens_in, dens_tile, dens_all, local, work, table,
    load_sems, sa, ra, sb, rb, sc, rc, sd, rd, sn, rn, st, rt, *held,
):
    band = lax.axis_index("band")
    slab = lax.axis_index("slab")

    loads = [
        pltpu.make_async_copy(a, b, load_sems.at[i])
        for i, (a, b) in enumerate(
            (
                (orb_hbm, orb), (partners_hbm, partners), (counts_hbm, counts),
                (dft_hbm, dft),
            )
        )
    ]
    for load in loads:
        load.start()

    def peer(me, i):
        return lax.rem(me + i, N)

    def each_peer(fn):
        def step(i, carry):
            fn(i)
            return carry

        lax.fori_loop(1, N, step, 0)

    barrier = pltpu.get_barrier_semaphore()

    def greet(i):
        pl.semaphore_signal(barrier, inc=1, device_id={"band": peer(band, i)}, device_id_type=MESH)
        pl.semaphore_signal(barrier, inc=1, device_id={"slab": peer(slab, i)}, device_id_type=MESH)

    each_peer(greet)
    loads[0].wait()

    for plane in range(3):
        for chunk in range(18):
            tile = orb[plane, :, chunk * LANES : (chunk + 1) * LANES]
            src[pl.ds(plane * 18 + chunk, N, stride=BLK), :] = tile
            dens[pl.ds(plane * 18 + chunk, 1), :] = jnp.sum(tile * tile, axis=0, keepdims=True)
    pl.semaphore_wait(barrier, 2 * (N - 1))

    def remote(a, b, send, recv, axis, p):
        return pltpu.make_async_remote_copy(
            src_ref=a, dst_ref=b, send_sem=send, recv_sem=recv,
            device_id={axis: p}, device_id_type=MESH,
        )

    def orbital_copy(c, p, at):
        first, count = CHUNKS[c]
        return remote(
            src.at[rows_of(p, first, count)], held[c].at[at],
            sa.at[c * N + p], ra.at[c * N + at], "band", p,
        )

    def tile_of(index):
        return pl.ds(pl.multiple_of(index * 8, 8), 8)

    def square_copy(p, tile, at):
        return remote(dens.at[tile_of(tile)], dens_in.at[tile_of(at)], sn.at[p], rn.at[at], "band", p)

    def density_copy(p, tile):
        return remote(dens_tile, dens_all.at[tile_of(tile)], st.at[p], rt.at[tile], "band", p)

    def if_summing(index, fn):
        pl.when(index < TILES)(fn)

    def pair_copy(k, c, p, at):
        first, count = CHUNKS[c]
        sem = (k * PARTS + c) * N
        return remote(
            pairs.at[rows_of(k * N + p, first, count)], tasks.at[rows_of(k * N + at, first, count)],
            sb.at[sem + p], rb.at[sem + at], "slab", p,
        )

    def pot_copy(k, c, p, at):
        first, count = CHUNKS[c]
        sem = (k * PARTS + c) * N
        return remote(
            pots.at[rows_of(k * N + p, first, count)], back.at[rows_of(k * N + at, first, count)],
            sc.at[sem + p], rc.at[sem + at], "slab", p,
        )

    def exchange_copy(c, p, at):
        first, count = CHUNKS[c]
        return remote(
            partial.at[rows_of(p, first, count)], final.at[rows_of(at, first, count)],
            sd.at[c * N + p], rd.at[c * N + at], "band", p,
        )

    for c in range(PARTS):
        each_peer(lambda i, c=c: orbital_copy(c, peer(band, i), band).start())
    for c, (first, count) in enumerate(CHUNKS):
        held[c][band] = src[rows_of(band, first, count), :]

    def to_summing(i):
        p = peer(band, i)
        if_summing(p, lambda: square_copy(p, p, band).start())

    each_peer(to_summing)

    @pl.when(band < TILES)
    def _():
        dens_in[tile_of(band), :] = dens[tile_of(band), :]

    fill_table(table)
    loads[1].wait()
    loads[2].wait()

    for c, (first, count) in enumerate(CHUNKS):
        each_peer(lambda i, c=c: orbital_copy(c, peer(band, i), peer(band, i)).wait_recv())
        for g in range(N):
            mine = held[c][g]
            for k in range(2):
                active = jnp.where(band < counts[k, g], 1.0, 0.0).astype(F32)
                product = mine * held[c][partners[k, g]] * active
                pairs[pl.ds((k * N + g) * BLK + first, count), :] = product
        for k in range(2):
            each_peer(lambda i, k=k, c=c: pair_copy(k, c, peer(slab, i), slab).start())
            at = rows_of(k * N + slab, first, count)
            tasks[at, :] = pairs[at, :]

    @pl.when(band < TILES)
    def _():
        each_peer(lambda i: square_copy(peer(band, i), band, peer(band, i)).wait_recv())
        summed = dens_in[0:8, :]
        for b in range(1, N):
            summed = summed + dens_in[b * 8 : (b + 1) * 8, :]
        dens_tile[...] = summed
        dens_all[tile_of(band), :] = summed
        each_peer(lambda i: density_copy(peer(band, i), band).start())

    for load in loads[3:]:
        load.wait()

    for k in range(2):
        for c in range(PARTS):
            each_peer(lambda i, k=k, c=c: pair_copy(k, c, peer(slab, i), peer(slab, i)).wait_recv())
        convolve(tasks, pots, k * N * BLK, work, table, dft)
        for c in range(PARTS):
            each_peer(lambda i, k=k, c=c: pot_copy(k, c, peer(slab, i), slab).start())
        back[block(k * N + slab), :] = pots[block(k * N + slab), :]

    def from_summing(i):
        p = peer(band, i)
        if_summing(p, lambda: density_copy(p, p).wait_recv())

    each_peer(from_summing)
    total = dens_all[...]
    total = total * (2.0 / (N * N))
    safe = jnp.maximum(total, 1e-37)
    root = jnp.exp(jnp.log(safe) * (1.0 / 3.0))
    root = root * (2.0 + safe / (root * root * root)) * (1.0 / 3.0)
    local[...] = SLATER * jnp.where(total > 0.0, root, 0.0)

    row = lax.broadcasted_iota(jnp.int32, (N, PAIRS), 0)
    col = lax.broadcasted_iota(jnp.int32, (N, PAIRS), 1)
    names = jnp.full((N, PAIRS), -1, jnp.int32)
    for k in range(2):
        for g in range(N):
            names = jnp.where(col == k * N + g, partners[k, g], names)
    onehot = jnp.where(names == row, 1.0, 0.0).astype(BF16)
    onehot3 = jnp.concatenate([onehot, onehot, onehot], axis=1)

    for c, (first, count) in enumerate(CHUNKS):
        for k in range(2):
            each_peer(lambda i, k=k, c=c: pot_copy(k, c, peer(slab, i), peer(slab, i)).wait_recv())

        for g in range(N):
            phi = held[c][g]
            own = jnp.zeros((count, LANES), F32)
            for k in range(2):
                at = pl.ds((k * N + g) * BLK + first, count)
                pot = back[at, :]
                own = own + pot * held[c][partners[k, g]]
                ret[at, :] = pot * phi
            partial[pl.ds(g * BLK + first, count), :] = own
        for eight in range(first, first + count, 8):
            wide = jnp.concatenate(
                [ret[pl.ds(eight + u, PAIRS, stride=BLK), :] for u in range(8)], axis=1
            )
            hi, mid = split(wide)
            low = (wide - hi.astype(F32) - mid.astype(F32)).astype(BF16)
            summed = dot(onehot3, jnp.concatenate([hi, mid, low], axis=0))
            for u in range(min(8, ROWS - eight)):
                at = pl.ds(eight + u, N, stride=BLK)
                partial[at, :] = -MIX * (partial[at, :] + summed[:, u * LANES : (u + 1) * LANES])
        if c == PARTS - 1:
            index_energy = jnp.sum(back[pl.ds(ROWS, PAIRS, stride=BLK), :], axis=0, keepdims=True)
            partial[pl.ds(ROWS, N, stride=BLK), :] = jnp.broadcast_to(index_energy, (N, LANES))
        each_peer(lambda i, c=c: exchange_copy(c, peer(band, i), band).start())
        final[rows_of(band, first, count), :] = partial[rows_of(band, first, count), :]

    def summing_left(i):
        p = peer(band, i)
        if_summing(p, lambda: square_copy(p, p, band).wait_send())

    each_peer(summing_left)
    if_summing(band, lambda: each_peer(lambda i: density_copy(peer(band, i), band).wait_send()))
    for c in range(PARTS):
        each_peer(lambda i, c=c: orbital_copy(c, peer(band, i), band).wait_send())
        for k in range(2):
            each_peer(lambda i, k=k, c=c: pair_copy(k, c, peer(slab, i), slab).wait_send())
            each_peer(lambda i, k=k, c=c: pot_copy(k, c, peer(slab, i), slab).wait_send())

    for c, (first, count) in enumerate(CHUNKS):
        each_peer(lambda i, c=c: exchange_copy(c, peer(band, i), peer(band, i)).wait_recv())
        for r in range(first, min(ROWS, first + count)):
            plane, chunk = divmod(r, 18)
            lanes = slice(chunk * LANES, (chunk + 1) * LANES)
            forces[plane, :, lanes] = (
                local[pl.ds(r, 1), :] * orb[plane, :, lanes] + final[pl.ds(r, N, stride=BLK), :]
            )
    energies = final[pl.ds(ROWS, N, stride=BLK), :]
    energy_out[0, 0] = jnp.sum(energies) * (-1.0 / (2.0 * N * N * NX * NY * NZ))
    for c in range(PARTS):
        each_peer(lambda i, c=c: exchange_copy(c, peer(band, i), band).wait_send())


def solution(mesh):
    dft = constants()
    vmem = pl.BlockSpec(memory_space=pltpu.VMEM)
    smem = pl.BlockSpec(memory_space=pltpu.SMEM)
    hbm = pl.BlockSpec(memory_space=pl.ANY)
    one = pltpu.VMEM((N * BLK, LANES), F32)
    two = pltpu.VMEM((2 * N * BLK, LANES), F32)
    line = pltpu.VMEM((BLK, LANES), F32)
    grid = pltpu.VMEM((48 * 48, LANES), F32)
    sems = lambda n: pltpu.SemaphoreType.DMA((n,))

    def body(orbitals, partners, counts):
        forces, energy = pl.pallas_call(
            kernel,
            out_shape=(
                jax.ShapeDtypeStruct((3, N, NY * NZ), F32),
                jax.ShapeDtypeStruct((1, 1), F32),
            ),
            in_specs=[hbm] * 4,
            out_specs=(vmem, smem),
            scratch_shapes=[
                pltpu.VMEM((3, N, NY * NZ), F32),
                pltpu.SMEM((2, N), jnp.int32),
                pltpu.SMEM((2, N), jnp.int32),
                pltpu.VMEM(dft.shape, BF16),
                one,
                two, two, two, two,
                one, one,
                two,
                line, pltpu.VMEM((N * 8, LANES), F32),
                pltpu.VMEM((8, LANES), F32), line, line,
                grid, grid,
                sems(4),
                sems(PARTS * N), sems(PARTS * N),
                sems(2 * PARTS * N), sems(2 * PARTS * N),
                sems(2 * PARTS * N), sems(2 * PARTS * N),
                sems(PARTS * N), sems(PARTS * N),
                sems(N), sems(N),
                sems(N), sems(N),
                *[pltpu.VMEM((N, count, LANES), F32) for _, count in CHUNKS],
            ],
            compiler_params=pltpu.CompilerParams(
                collective_id=0, has_side_effects=True, vmem_limit_bytes=VMEM_BYTES
            ),
        )(
            orbitals.transpose(1, 0, 2), partners.T, counts.T,
            jnp.asarray(dft),
        )
        return forces.transpose(1, 0, 2), energy.reshape(())

    specs = P("band", "slab", None)
    return jax.shard_map(
        body, mesh=mesh, in_specs=(specs, P(), P()), out_specs=(specs, P()), check_vma=False
    )
```

```python
import functools
import math

import jax
import jax.numpy as jnp
import numpy as np
from jax import lax
from jax.experimental import pallas as pl
from jax.experimental.pallas import tpu as pltpu
from jax.sharding import PartitionSpec as P

NX = 48
NY = 48
NZ = 48
NZP = 96
N = 16
ROWS = 54
BLK = 56
LANES = 128
CHUNKS = ((0, BLK),)
PARTS = len(CHUNKS)
TILES = BLK // 8
PAIRS = 2 * N
SLATER = -((3.0 / math.pi) ** (1.0 / 3.0))
MIX = 0.25
VMEM_BYTES = 56_000_000
SCREENING = 0.25
F32 = jnp.float32
BF16 = jnp.bfloat16
MESH = pl.DeviceIdType.MESH


def split_np(w):
    hi = w.astype(np.float32).astype(jnp.bfloat16)
    lo = (w - hi.astype(np.float64)).astype(np.float32).astype(jnp.bfloat16)
    return hi, lo


def cas(length):
    j = np.arange(length)
    angle = 2.0 * np.pi * ((j[:, None] * j[None, :]) % length) / length
    return (np.cos(angle) + np.sin(angle)) / np.sqrt(length)


def constants():
    h = cas(48)
    order = np.array([3 * p + plane for plane in range(3) for p in range(16)])
    wx = h[:, order]

    def left(w):
        hi, lo = split_np(w)
        return np.concatenate([hi, hi, lo], axis=1)

    small = np.stack([left(wx), left(h), left(wx.T)])
    hz = cas(NZP)[:NZ, :]
    full = np.zeros((384, 8, LANES))
    for y8 in range(8):
        full[y8 * 48 : (y8 + 1) * 48, y8, :NZP] = hz
    full = full.reshape(384, 8 * LANES)
    fwd = np.concatenate(
        [full[0:128, 0:256], full[0:256, 256:512], full[128:384, 512:768], full[256:384, 768:1024]]
    )
    back = full.T
    inv01 = back[0 : 6 * 128, 0:256]
    inv2 = back[5 * 128 : 8 * 128, 256:384]
    small = np.pad(small.reshape(144, 144), ((0, 0), (0, 112)))
    return np.concatenate(
        [*split_np(fwd), *split_np(inv01), np.concatenate(split_np(inv2), axis=1), small]
    )


def split(x):
    hi = x.astype(BF16)
    lo = (x - hi.astype(F32)).astype(BF16)
    return hi, lo


def dot(a, b):
    return jnp.dot(a, b, preferred_element_type=F32)


def dot3(x_hl, w_hi, w_lo, m):
    both = dot(x_hl, w_hi)
    return both[:m] + both[m:] + dot(x_hl[:m], w_lo)


def left3(w3, x):
    hi, lo = split(x)
    return dot(w3, jnp.concatenate([hi, lo, hi], axis=0))


def fill_table(table):
    def wave_sq(index, length):
        signed = jnp.where(index > length // 2, index - length, index).astype(F32)
        wave = 2.0 * math.pi / length * signed
        return wave * wave

    lane = lax.broadcasted_iota(jnp.int32, (48, LANES), 1)
    row = lax.broadcasted_iota(jnp.int32, (48, LANES), 0)
    yz = wave_sq(row, NY) + wave_sq(lane, NZP) + SCREENING * SCREENING

    def step(qx, carry):
        wx = wave_sq(jnp.full((48, LANES), qx, jnp.int32), NX)
        value = jnp.where(lane < NZP, 4.0 * math.pi / (yz + wx), 0.0)
        table[pl.ds(pl.multiple_of(qx * 48, 8), 48), :] = value
        return carry

    lax.fori_loop(0, 48, step, 0)


def convolve(pd, pot, base, work, table, dft):
    rows = 288

    def gather(ref, t):
        tiles = [
            ref[pl.ds(base + plane * 18 + yg * 3 + t, 16, stride=BLK), :]
            for yg in range(6)
            for plane in range(3)
        ]
        return jnp.concatenate(tiles, axis=0)

    def scatter_z(j, value):
        for yg in range(6):
            for half in range(2):
                y = yg * 8 + 2 * j + half
                work[pl.ds(y * 48, 48), :] = value[
                    yg * 48 : (yg + 1) * 48, half * LANES : (half + 1) * LANES
                ]

    def stack(t):
        hi, lo = split(gather(pd, t))
        return jnp.concatenate([hi, lo], axis=0)

    s0 = stack(0)
    scatter_z(0, dot3(s0, dft[0:128], dft[768 : 768 + 128], rows))
    s1 = stack(1)
    s01 = jnp.concatenate([s0, s1], axis=1)
    scatter_z(1, dot3(s01, dft[128:384], dft[768 + 128 : 768 + 384], rows))
    s2 = stack(2)
    s12 = jnp.concatenate([s1, s2], axis=1)
    scatter_z(2, dot3(s12, dft[384:640], dft[768 + 384 : 768 + 640], rows))
    scatter_z(3, dot3(s2, dft[640:768], dft[768 + 640 : 768 + 768], rows))

    def along_x(which):
        w3 = dft[3456 + 48 * which : 3504 + 48 * which, 0:144]

        def step(i, carry):
            start = pl.multiple_of(i * 384, 8)
            block = work[pl.ds(start, 384), :]
            wide = jnp.concatenate([block[48 * u : 48 * (u + 1)] for u in range(8)], axis=1)
            out = left3(w3, wide)
            work[pl.ds(start, 384), :] = jnp.concatenate(
                [out[:, LANES * u : LANES * (u + 1)] for u in range(8)], axis=0
            )
            return carry

        lax.fori_loop(0, 6, step, 0, unroll=6)

    along_x(0)
    wy3 = dft[3504:3552, 0:144]

    def y_step(i, carry):
        qx = i * 8
        wide = jnp.concatenate(
            [work[pl.ds(qx + u, 48, stride=48), :] for u in range(8)], axis=1
        )
        spectrum = left3(wy3, wide)
        k = table[pl.ds(pl.multiple_of(qx * 48, 8), 384), :]
        k = jnp.concatenate([k[48 * u : 48 * (u + 1)] for u in range(8)], axis=1)
        out = left3(wy3, spectrum * k)
        for u in range(8):
            work[pl.ds(qx + u, 48, stride=48), :] = out[:, LANES * u : LANES * (u + 1)]
        return carry

    lax.fori_loop(0, 6, y_step, 0, unroll=6)
    along_x(2)

    def gather_y8(y8):
        tiles = [work[pl.ds((yg * 8 + y8) * 48, 48), :] for yg in range(6)]
        hi, lo = split(jnp.concatenate(tiles, axis=0))
        return jnp.concatenate([hi, lo], axis=0)

    energy = jnp.zeros((16, LANES), F32)

    def scatter_t(t, value, energy):
        for yg in range(6):
            for plane in range(3):
                at = pl.ds(base + plane * 18 + yg * 3 + t, 16, stride=BLK)
                tile = value[(yg * 3 + plane) * 16 : (yg * 3 + plane + 1) * 16]
                pot[at, :] = tile
                energy = energy + tile * pd[at, :]
        return energy

    parts = [gather_y8(y8) for y8 in range(6)]
    first = jnp.concatenate(parts, axis=1)
    out = dot3(first, dft[1536:2304], dft[2304:3072], rows)
    energy = scatter_t(0, out[:, 0:128], energy)
    energy = scatter_t(1, out[:, 128:256], energy)
    second = jnp.concatenate([parts[5], gather_y8(6), gather_y8(7)], axis=1)
    energy = scatter_t(2, dot3(second, dft[3072:3456, 0:128], dft[3072:3456, 128:256], rows), energy)
    total = jnp.sum(energy, axis=0, keepdims=True)
    pot[pl.ds(base + ROWS, 16, stride=BLK), :] = jnp.broadcast_to(total, (16, LANES))


def rows_of(index, first, count):
    return pl.ds(pl.multiple_of(index * BLK + first, 8), count)


def block(index):
    return rows_of(index, 0, BLK)


def kernel(
    orb_hbm, partners_hbm, counts_hbm, dft_hbm,
    forces, energy_out,
    orb, partners, counts, dft,
    src, pairs, tasks, pots, back, partial, final, ret, dens, dens_in, dens_tile, dens_all, local, work, table,
    load_sems, sa, ra, sb, rb, sc, rc, sd, rd, sn, rn, st, rt, *held,
):
    band = lax.axis_index("band")
    slab = lax.axis_index("slab")

    loads = [
        pltpu.make_async_copy(a, b, load_sems.at[i])
        for i, (a, b) in enumerate(
            (
                (orb_hbm, orb), (partners_hbm, partners), (counts_hbm, counts),
                (dft_hbm, dft),
            )
        )
    ]
    for load in loads:
        load.start()

    def peer(me, i):
        j = i - 1
        if me is band:
            h = j // 2
            dz = 4 + lax.rem(h, 2) * -((h + 1) // 2) + (1 - lax.rem(h, 2)) * (h // 2)
            bx = lax.rem(band // 8 + 1 - lax.rem(j, 2), 2)
            return bx * 8 + lax.rem(lax.rem(band, 8) + dz, 8)
        h = j // 4
        dy = jnp.where(h == 0, 2, jnp.where(h == 1, 1, jnp.where(h == 2, 3, 0)))
        low = lax.bitwise_xor(lax.rem(slab, 4), 3 - lax.rem(j, 4))
        return lax.rem(slab // 4 + dy, 4) * 4 + low

    def each_peer(fn):
        def step(i, carry):
            fn(i)
            return carry

        lax.fori_loop(1, N, step, 0)

    barrier = pltpu.get_barrier_semaphore()

    def greet(i):
        pl.semaphore_signal(barrier, inc=1, device_id={"band": peer(band, i)}, device_id_type=MESH)
        pl.semaphore_signal(barrier, inc=1, device_id={"slab": peer(slab, i)}, device_id_type=MESH)

    each_peer(greet)
    loads[0].wait()

    for plane in range(3):
        for chunk in range(18):
            tile = orb[plane, :, chunk * LANES : (chunk + 1) * LANES]
            src[pl.ds(plane * 18 + chunk, N, stride=BLK), :] = tile
            dens[pl.ds(plane * 18 + chunk, 1), :] = jnp.sum(tile * tile, axis=0, keepdims=True)
    pl.semaphore_wait(barrier, 2 * (N - 1))

    def remote(a, b, send, recv, axis, p):
        return pltpu.make_async_remote_copy(
            src_ref=a, dst_ref=b, send_sem=send, recv_sem=recv,
            device_id={axis: p}, device_id_type=MESH,
        )

    def orbital_copy(c, p, at):
        first, count = CHUNKS[c]
        return remote(
            src.at[rows_of(p, first, count)], held[c].at[at],
            sa.at[c * N + p], ra.at[c * N + at], "band", p,
        )

    def tile_of(index):
        return pl.ds(pl.multiple_of(index * 8, 8), 8)

    def square_copy(p, tile, at):
        return remote(dens.at[tile_of(tile)], dens_in.at[tile_of(at)], sn.at[p], rn.at[at], "band", p)

    def density_copy(p, tile):
        return remote(dens_tile, dens_all.at[tile_of(tile)], st.at[p], rt.at[tile], "band", p)

    def if_summing(index, fn):
        pl.when(index < TILES)(fn)

    def pair_copy(k, c, p, at):
        first, count = CHUNKS[c]
        sem = (k * PARTS + c) * N
        return remote(
            pairs.at[rows_of(k * N + p, first, count)], tasks.at[rows_of(k * N + at, first, count)],
            sb.at[sem + p], rb.at[sem + at], "slab", p,
        )

    def pot_copy(k, c, p, at):
        first, count = CHUNKS[c]
        sem = (k * PARTS + c) * N
        return remote(
            pots.at[rows_of(k * N + p, first, count)], back.at[rows_of(k * N + at, first, count)],
            sc.at[sem + p], rc.at[sem + at], "slab", p,
        )

    def exchange_copy(c, p, at):
        first, count = CHUNKS[c]
        return remote(
            partial.at[rows_of(p, first, count)], final.at[rows_of(at, first, count)],
            sd.at[c * N + p], rd.at[c * N + at], "band", p,
        )

    for c in range(PARTS):
        each_peer(lambda i, c=c: orbital_copy(c, peer(band, i), band).start())
    for c, (first, count) in enumerate(CHUNKS):
        held[c][band] = src[rows_of(band, first, count), :]

    def to_summing(i):
        p = peer(band, i)
        if_summing(p, lambda: square_copy(p, p, band).start())

    each_peer(to_summing)

    @pl.when(band < TILES)
    def _():
        dens_in[tile_of(band), :] = dens[tile_of(band), :]

    fill_table(table)
    loads[1].wait()
    loads[2].wait()

    for c, (first, count) in enumerate(CHUNKS):
        each_peer(lambda i, c=c: orbital_copy(c, peer(band, i), peer(band, i)).wait_recv())
        for g in range(N):
            mine = held[c][g]
            for k in range(2):
                active = jnp.where(band < counts[k, g], 1.0, 0.0).astype(F32)
                product = mine * held[c][partners[k, g]] * active
                pairs[pl.ds((k * N + g) * BLK + first, count), :] = product
        for k in range(2):
            if k == 0:
                each_peer(lambda i, k=k, c=c: pair_copy(k, c, peer(slab, i), slab).start())
            at = rows_of(k * N + slab, first, count)
            tasks[at, :] = pairs[at, :]

    @pl.when(band < TILES)
    def _():
        each_peer(lambda i: square_copy(peer(band, i), band, peer(band, i)).wait_recv())
        summed = dens_in[0:8, :]
        for b in range(1, N):
            summed = summed + dens_in[b * 8 : (b + 1) * 8, :]
        dens_tile[...] = summed
        dens_all[tile_of(band), :] = summed
        each_peer(lambda i: density_copy(peer(band, i), band).start())

    for load in loads[3:]:
        load.wait()

    for k in range(2):
        for c in range(PARTS):
            def pair_in(i, k=k, c=c):
                p = peer(slab, i)
                pair_copy(k, c, p, p).wait_recv()
                if k == 0:
                    pair_copy(1, c, p, slab).start()

            each_peer(pair_in)
        convolve(tasks, pots, k * N * BLK, work, table, dft)
        for c in range(PARTS):
            each_peer(lambda i, k=k, c=c: pot_copy(k, c, peer(slab, i), slab).start())
        back[block(k * N + slab), :] = pots[block(k * N + slab), :]

    def from_summing(i):
        p = peer(band, i)
        if_summing(p, lambda: density_copy(p, p).wait_recv())

    each_peer(from_summing)
    total = dens_all[...]
    total = total * (2.0 / (N * N))
    safe = jnp.maximum(total, 1e-37)
    root = jnp.exp(jnp.log(safe) * (1.0 / 3.0))
    root = root * (2.0 + safe / (root * root * root)) * (1.0 / 3.0)
    local[...] = SLATER * jnp.where(total > 0.0, root, 0.0)

    row = lax.broadcasted_iota(jnp.int32, (N, PAIRS), 0)
    col = lax.broadcasted_iota(jnp.int32, (N, PAIRS), 1)
    names = jnp.full((N, PAIRS), -1, jnp.int32)
    for k in range(2):
        for g in range(N):
            names = jnp.where(col == k * N + g, partners[k, g], names)
    onehot = jnp.where(names == row, 1.0, 0.0).astype(BF16)
    onehot3 = jnp.concatenate([onehot, onehot, onehot], axis=1)

    for c, (first, count) in enumerate(CHUNKS):
        for k in range(2):
            each_peer(lambda i, k=k, c=c: pot_copy(k, c, peer(slab, i), peer(slab, i)).wait_recv())

        for g in range(N):
            phi = held[c][g]
            own = jnp.zeros((count, LANES), F32)
            for k in range(2):
                at = pl.ds((k * N + g) * BLK + first, count)
                pot = back[at, :]
                own = own + pot * held[c][partners[k, g]]
                ret[at, :] = pot * phi
            partial[pl.ds(g * BLK + first, count), :] = own
        for eight in range(first, first + count, 8):
            wide = jnp.concatenate(
                [ret[pl.ds(eight + u, PAIRS, stride=BLK), :] for u in range(8)], axis=1
            )
            hi, mid = split(wide)
            low = (wide - hi.astype(F32) - mid.astype(F32)).astype(BF16)
            summed = dot(onehot3, jnp.concatenate([hi, mid, low], axis=0))
            for u in range(min(8, ROWS - eight)):
                at = pl.ds(eight + u, N, stride=BLK)
                partial[at, :] = -MIX * (partial[at, :] + summed[:, u * LANES : (u + 1) * LANES])
        if c == PARTS - 1:
            index_energy = jnp.sum(back[pl.ds(ROWS, PAIRS, stride=BLK), :], axis=0, keepdims=True)
            partial[pl.ds(ROWS, N, stride=BLK), :] = jnp.broadcast_to(index_energy, (N, LANES))
        each_peer(lambda i, c=c: exchange_copy(c, peer(band, i), band).start())
        final[rows_of(band, first, count), :] = partial[rows_of(band, first, count), :]

    def summing_left(i):
        p = peer(band, i)
        if_summing(p, lambda: square_copy(p, p, band).wait_send())

    each_peer(summing_left)
    if_summing(band, lambda: each_peer(lambda i: density_copy(peer(band, i), band).wait_send()))
    for c in range(PARTS):
        each_peer(lambda i, c=c: orbital_copy(c, peer(band, i), band).wait_send())
        for k in range(2):
            each_peer(lambda i, k=k, c=c: pair_copy(k, c, peer(slab, i), slab).wait_send())
            each_peer(lambda i, k=k, c=c: pot_copy(k, c, peer(slab, i), slab).wait_send())

    for c, (first, count) in enumerate(CHUNKS):
        each_peer(lambda i, c=c: exchange_copy(c, peer(band, i), peer(band, i)).wait_recv())
        for r in range(first, min(ROWS, first + count)):
            plane, chunk = divmod(r, 18)
            lanes = slice(chunk * LANES, (chunk + 1) * LANES)
            forces[plane, :, lanes] = (
                local[pl.ds(r, 1), :] * orb[plane, :, lanes] + final[pl.ds(r, N, stride=BLK), :]
            )
    energies = final[pl.ds(ROWS, N, stride=BLK), :]
    energy_out[0, 0] = jnp.sum(energies) * (-1.0 / (2.0 * N * N * NX * NY * NZ))
    for c in range(PARTS):
        each_peer(lambda i, c=c: exchange_copy(c, peer(band, i), band).wait_send())


def solution(mesh):
    dft = constants()
    vmem = pl.BlockSpec(memory_space=pltpu.VMEM)
    smem = pl.BlockSpec(memory_space=pltpu.SMEM)
    hbm = pl.BlockSpec(memory_space=pl.ANY)
    one = pltpu.VMEM((N * BLK, LANES), F32)
    two = pltpu.VMEM((2 * N * BLK, LANES), F32)
    line = pltpu.VMEM((BLK, LANES), F32)
    grid = pltpu.VMEM((48 * 48, LANES), F32)
    sems = lambda n: pltpu.SemaphoreType.DMA((n,))

    def body(orbitals, partners, counts):
        forces, energy = pl.pallas_call(
            kernel,
            out_shape=(
                jax.ShapeDtypeStruct((3, N, NY * NZ), F32),
                jax.ShapeDtypeStruct((1, 1), F32),
            ),
            in_specs=[hbm] * 4,
            out_specs=(vmem, smem),
            scratch_shapes=[
                pltpu.VMEM((3, N, NY * NZ), F32),
                pltpu.SMEM((2, N), jnp.int32),
                pltpu.SMEM((2, N), jnp.int32),
                pltpu.VMEM(dft.shape, BF16),
                one,
                two, two, two, two,
                one, one,
                two,
                line, pltpu.VMEM((N * 8, LANES), F32),
                pltpu.VMEM((8, LANES), F32), line, line,
                grid, grid,
                sems(4),
                sems(PARTS * N), sems(PARTS * N),
                sems(2 * PARTS * N), sems(2 * PARTS * N),
                sems(2 * PARTS * N), sems(2 * PARTS * N),
                sems(PARTS * N), sems(PARTS * N),
                sems(N), sems(N),
                sems(N), sems(N),
                *[pltpu.VMEM((N, count, LANES), F32) for _, count in CHUNKS],
            ],
            compiler_params=pltpu.CompilerParams(
                collective_id=0, has_side_effects=True, vmem_limit_bytes=VMEM_BYTES
            ),
        )(
            orbitals.transpose(1, 0, 2), partners.T, counts.T,
            jnp.asarray(dft),
        )
        return forces.transpose(1, 0, 2), energy.reshape(())

    specs = P("band", "slab", None)
    return jax.shard_map(
        body, mesh=mesh, in_specs=(specs, P(), P()), out_specs=(specs, P()), check_vma=False
    )
```

```python
import functools
import math

import jax
import jax.numpy as jnp
import numpy as np
from jax import lax
from jax.experimental import pallas as pl
from jax.experimental.pallas import tpu as pltpu
from jax.sharding import PartitionSpec as P

NX = 48
NY = 48
NZ = 48
NZP = 96
N = 16
ROWS = 54
BLK = 56
LANES = 128
CHUNKS = ((0, BLK),)
PARTS = len(CHUNKS)
TILES = BLK // 8
PAIRS = 2 * N
SLATER = -((3.0 / math.pi) ** (1.0 / 3.0))
MIX = 0.25
VMEM_BYTES = 56_000_000
SCREENING = 0.25
F32 = jnp.float32
BF16 = jnp.bfloat16
MESH = pl.DeviceIdType.MESH


def split_np(w):
    hi = w.astype(np.float32).astype(jnp.bfloat16)
    lo = (w - hi.astype(np.float64)).astype(np.float32).astype(jnp.bfloat16)
    return hi, lo


def cas(length):
    j = np.arange(length)
    angle = 2.0 * np.pi * ((j[:, None] * j[None, :]) % length) / length
    return (np.cos(angle) + np.sin(angle)) / np.sqrt(length)


def constants():
    h = cas(48)
    order = np.array([3 * p + plane for plane in range(3) for p in range(16)])
    wx = h[:, order]

    def left(w):
        hi, lo = split_np(w)
        return np.concatenate([hi, hi, lo], axis=1)

    small = np.stack([left(wx), left(h), left(wx.T)])
    hz = cas(NZP)[:NZ, :]
    full = np.zeros((384, 8, LANES))
    for y8 in range(8):
        full[y8 * 48 : (y8 + 1) * 48, y8, :NZP] = hz
    full = full.reshape(384, 8 * LANES)
    fwd = np.concatenate(
        [full[0:128, 0:256], full[0:256, 256:512], full[128:384, 512:768], full[256:384, 768:1024]]
    )
    back = full.T
    inv01 = back[0 : 6 * 128, 0:256]
    inv2 = back[5 * 128 : 8 * 128, 256:384]
    small = np.pad(small.reshape(144, 144), ((0, 0), (0, 112)))
    return np.concatenate(
        [*split_np(fwd), *split_np(inv01), np.concatenate(split_np(inv2), axis=1), small]
    )


def split(x):
    hi = x.astype(BF16)
    lo = (x - hi.astype(F32)).astype(BF16)
    return hi, lo


def dot(a, b):
    return jnp.dot(a, b, preferred_element_type=F32)


def dot3(x_hl, w_hi, w_lo, m):
    both = dot(x_hl, w_hi)
    return both[:m] + both[m:] + dot(x_hl[:m], w_lo)


def left3(w3, x):
    hi, lo = split(x)
    return dot(w3, jnp.concatenate([hi, lo, hi], axis=0))


def fill_table(table):
    def wave_sq(index, length):
        signed = jnp.where(index > length // 2, index - length, index).astype(F32)
        wave = 2.0 * math.pi / length * signed
        return wave * wave

    lane = lax.broadcasted_iota(jnp.int32, (48, LANES), 1)
    row = lax.broadcasted_iota(jnp.int32, (48, LANES), 0)
    yz = wave_sq(row, NY) + wave_sq(lane, NZP) + SCREENING * SCREENING

    def step(qx, carry):
        wx = wave_sq(jnp.full((48, LANES), qx, jnp.int32), NX)
        value = jnp.where(lane < NZP, 4.0 * math.pi / (yz + wx), 0.0)
        table[pl.ds(pl.multiple_of(qx * 48, 8), 48), :] = value
        return carry

    lax.fori_loop(0, 48, step, 0)


def convolve(pd, pot, base, work, table, dft):
    rows = 288

    def gather(ref, t):
        tiles = [
            ref[pl.ds(base + plane * 18 + yg * 3 + t, 16, stride=BLK), :]
            for yg in range(6)
            for plane in range(3)
        ]
        return jnp.concatenate(tiles, axis=0)

    def scatter_z(j, value):
        for yg in range(6):
            for half in range(2):
                y = yg * 8 + 2 * j + half
                work[pl.ds(y * 48, 48), :] = value[
                    yg * 48 : (yg + 1) * 48, half * LANES : (half + 1) * LANES
                ]

    def stack(t):
        hi, lo = split(gather(pd, t))
        return jnp.concatenate([hi, lo], axis=0)

    s0 = stack(0)
    scatter_z(0, dot3(s0, dft[0:128], dft[768 : 768 + 128], rows))
    s1 = stack(1)
    s01 = jnp.concatenate([s0, s1], axis=1)
    scatter_z(1, dot3(s01, dft[128:384], dft[768 + 128 : 768 + 384], rows))
    s2 = stack(2)
    s12 = jnp.concatenate([s1, s2], axis=1)
    scatter_z(2, dot3(s12, dft[384:640], dft[768 + 384 : 768 + 640], rows))
    scatter_z(3, dot3(s2, dft[640:768], dft[768 + 640 : 768 + 768], rows))

    def along_x(which):
        w3 = dft[3456 + 48 * which : 3504 + 48 * which, 0:144]

        def step(i, carry):
            start = pl.multiple_of(i * 384, 8)
            block = work[pl.ds(start, 384), :]
            wide = jnp.concatenate([block[48 * u : 48 * (u + 1)] for u in range(8)], axis=1)
            out = left3(w3, wide)
            work[pl.ds(start, 384), :] = jnp.concatenate(
                [out[:, LANES * u : LANES * (u + 1)] for u in range(8)], axis=0
            )
            return carry

        lax.fori_loop(0, 6, step, 0, unroll=6)

    along_x(0)
    wy3 = dft[3504:3552, 0:144]

    def y_step(i, carry):
        qx = i * 8
        wide = jnp.concatenate(
            [work[pl.ds(qx + u, 48, stride=48), :] for u in range(8)], axis=1
        )
        spectrum = left3(wy3, wide)
        k = table[pl.ds(pl.multiple_of(qx * 48, 8), 384), :]
        k = jnp.concatenate([k[48 * u : 48 * (u + 1)] for u in range(8)], axis=1)
        out = left3(wy3, spectrum * k)
        for u in range(8):
            work[pl.ds(qx + u, 48, stride=48), :] = out[:, LANES * u : LANES * (u + 1)]
        return carry

    lax.fori_loop(0, 6, y_step, 0, unroll=6)
    along_x(2)

    def gather_y8(y8):
        tiles = [work[pl.ds((yg * 8 + y8) * 48, 48), :] for yg in range(6)]
        hi, lo = split(jnp.concatenate(tiles, axis=0))
        return jnp.concatenate([hi, lo], axis=0)

    energy = jnp.zeros((16, LANES), F32)

    def scatter_t(t, value, energy):
        for yg in range(6):
            for plane in range(3):
                at = pl.ds(base + plane * 18 + yg * 3 + t, 16, stride=BLK)
                tile = value[(yg * 3 + plane) * 16 : (yg * 3 + plane + 1) * 16]
                pot[at, :] = tile
                energy = energy + tile * pd[at, :]
        return energy

    parts = [gather_y8(y8) for y8 in range(6)]
    first = jnp.concatenate(parts, axis=1)
    out = dot3(first, dft[1536:2304], dft[2304:3072], rows)
    energy = scatter_t(0, out[:, 0:128], energy)
    energy = scatter_t(1, out[:, 128:256], energy)
    second = jnp.concatenate([parts[5], gather_y8(6), gather_y8(7)], axis=1)
    energy = scatter_t(2, dot3(second, dft[3072:3456, 0:128], dft[3072:3456, 128:256], rows), energy)
    total = jnp.sum(energy, axis=0, keepdims=True)
    pot[pl.ds(base + ROWS, 16, stride=BLK), :] = jnp.broadcast_to(total, (16, LANES))


def rows_of(index, first, count):
    return pl.ds(pl.multiple_of(index * BLK + first, 8), count)


def block(index):
    return rows_of(index, 0, BLK)


def kernel(
    orb_hbm, partners_hbm, counts_hbm, dft_hbm,
    forces, energy_out,
    orb, partners, counts, dft,
    src, pairs, tasks, pots, back, partial, final, ret, dens, dens_in, dens_tile, dens_all, local, work, table,
    load_sems, sa, ra, sb, rb, sc, rc, sd, rd, sn, rn, st, rt, *held,
):
    band = lax.axis_index("band")
    slab = lax.axis_index("slab")

    loads = [
        pltpu.make_async_copy(a, b, load_sems.at[i])
        for i, (a, b) in enumerate(
            (
                (orb_hbm, orb), (partners_hbm, partners), (counts_hbm, counts),
                (dft_hbm, dft),
            )
        )
    ]
    for load in loads:
        load.start()

    def peer(me, i):
        j = i - 1
        if me is band:
            h = j // 2
            dz = 4 + lax.rem(h, 2) * -((h + 1) // 2) + (1 - lax.rem(h, 2)) * (h // 2)
            bx = lax.rem(band // 8 + 1 - lax.rem(j, 2), 2)
            return bx * 8 + lax.rem(lax.rem(band, 8) + dz, 8)
        h = j // 4
        dy = jnp.where(h == 0, 2, jnp.where(h == 1, 1, jnp.where(h == 2, 3, 0)))
        low = lax.bitwise_xor(lax.rem(slab, 4), 3 - lax.rem(j, 4))
        return lax.rem(slab // 4 + dy, 4) * 4 + low

    def each_peer(fn):
        def step(i, carry):
            fn(i)
            return carry

        lax.fori_loop(1, N, step, 0)

    barrier = pltpu.get_barrier_semaphore()

    def greet(i):
        pl.semaphore_signal(barrier, inc=1, device_id={"band": peer(band, i)}, device_id_type=MESH)
        pl.semaphore_signal(barrier, inc=1, device_id={"slab": peer(slab, i)}, device_id_type=MESH)

    each_peer(greet)
    loads[0].wait()

    for plane in range(3):
        for chunk in range(18):
            tile = orb[plane, :, chunk * LANES : (chunk + 1) * LANES]
            src[pl.ds(plane * 18 + chunk, N, stride=BLK), :] = tile
            dens[pl.ds(plane * 18 + chunk, 1), :] = jnp.sum(tile * tile, axis=0, keepdims=True)
    pl.semaphore_wait(barrier, 2 * (N - 1))

    def remote(a, b, send, recv, axis, p):
        return pltpu.make_async_remote_copy(
            src_ref=a, dst_ref=b, send_sem=send, recv_sem=recv,
            device_id={axis: p}, device_id_type=MESH,
        )

    def orbital_copy(c, p, at):
        first, count = CHUNKS[c]
        return remote(
            src.at[rows_of(p, first, count)], held[c].at[at],
            sa.at[c * N + p], ra.at[c * N + at], "band", p,
        )

    def tile_of(index):
        return pl.ds(pl.multiple_of(index * 8, 8), 8)

    def square_copy(p, tile, at):
        return remote(dens.at[tile_of(tile)], dens_in.at[tile_of(at)], sn.at[p], rn.at[at], "band", p)

    def density_copy(p, tile):
        return remote(dens_tile, dens_all.at[tile_of(tile)], st.at[p], rt.at[tile], "band", p)

    def if_summing(index, fn):
        pl.when(index < TILES)(fn)

    def pair_copy(k, c, p, at):
        first, count = CHUNKS[c]
        sem = (k * PARTS + c) * N
        return remote(
            pairs.at[rows_of(k * N + p, first, count)], tasks.at[rows_of(k * N + at, first, count)],
            sb.at[sem + p], rb.at[sem + at], "slab", p,
        )

    def pot_copy(k, c, p, at):
        first, count = CHUNKS[c]
        sem = (k * PARTS + c) * N
        return remote(
            pots.at[rows_of(k * N + p, first, count)], back.at[rows_of(k * N + at, first, count)],
            sc.at[sem + p], rc.at[sem + at], "slab", p,
        )

    def exchange_copy(c, p, at):
        first, count = CHUNKS[c]
        return remote(
            partial.at[rows_of(p, first, count)], final.at[rows_of(at, first, count)],
            sd.at[c * N + p], rd.at[c * N + at], "band", p,
        )

    for c in range(PARTS):
        each_peer(lambda i, c=c: orbital_copy(c, peer(band, i), band).start())
    for c, (first, count) in enumerate(CHUNKS):
        held[c][band] = src[rows_of(band, first, count), :]

    def to_summing(i):
        p = peer(band, i)
        if_summing(p, lambda: square_copy(p, p, band).start())

    each_peer(to_summing)

    @pl.when(band < TILES)
    def _():
        dens_in[tile_of(band), :] = dens[tile_of(band), :]

    fill_table(table)
    loads[1].wait()
    loads[2].wait()

    for c, (first, count) in enumerate(CHUNKS):
        each_peer(lambda i, c=c: orbital_copy(c, peer(band, i), peer(band, i)).wait_recv())
        for g in range(N):
            mine = held[c][g]
            for k in range(2):
                active = jnp.where(band < counts[k, g], 1.0, 0.0).astype(F32)
                product = mine * held[c][partners[k, g]] * active
                pairs[pl.ds((k * N + g) * BLK + first, count), :] = product
        for k in range(2):
            if k == 0:
                each_peer(lambda i, k=k, c=c: pair_copy(k, c, peer(slab, i), slab).start())
            at = rows_of(k * N + slab, first, count)
            tasks[at, :] = pairs[at, :]

    @pl.when(band < TILES)
    def _():
        each_peer(lambda i: square_copy(peer(band, i), band, peer(band, i)).wait_recv())
        summed = dens_in[0:8, :]
        for b in range(1, N):
            summed = summed + dens_in[b * 8 : (b + 1) * 8, :]
        dens_tile[...] = summed
        dens_all[tile_of(band), :] = summed
        each_peer(lambda i: density_copy(peer(band, i), band).start())

    for load in loads[3:]:
        load.wait()

    for k in range(2):
        for c in range(PARTS):
            def pair_in(i, k=k, c=c):
                p = peer(slab, i)
                pair_copy(k, c, p, p).wait_recv()
                if k == 0:
                    pair_copy(1, c, p, slab).start()

            each_peer(pair_in)
        convolve(tasks, pots, k * N * BLK, work, table, dft)
        for c in range(PARTS):
            each_peer(lambda i, k=k, c=c: pot_copy(k, c, peer(slab, i), slab).start())
        back[block(k * N + slab), :] = pots[block(k * N + slab), :]

    def from_summing(i):
        p = peer(band, i)
        if_summing(p, lambda: density_copy(p, p).wait_recv())

    each_peer(from_summing)
    total = dens_all[...]
    total = total * (2.0 / (N * N))
    safe = jnp.maximum(total, 1e-37)
    root = jnp.exp(jnp.log(safe) * (1.0 / 3.0))
    root = root * (2.0 + safe / (root * root * root)) * (1.0 / 3.0)
    local[...] = SLATER * jnp.where(total > 0.0, root, 0.0)

    row = lax.broadcasted_iota(jnp.int32, (N, N), 0)
    col = lax.broadcasted_iota(jnp.int32, (N, N), 1)
    onehots = []
    for k in range(2):
        names = jnp.full((N, N), -1, jnp.int32)
        for g in range(N):
            names = jnp.where(col == g, partners[k, g], names)
        onehot = jnp.where(names == row, 1.0, 0.0).astype(BF16)
        onehots.append(jnp.concatenate([onehot, onehot, onehot], axis=1))

    for c, (first, count) in enumerate(CHUNKS):
        for k in range(2):
            each_peer(lambda i, k=k, c=c: pot_copy(k, c, peer(slab, i), peer(slab, i)).wait_recv())
            for g in range(N):
                at = pl.ds((k * N + g) * BLK + first, count)
                to = pl.ds(g * BLK + first, count)
                pot = back[at, :]
                own = pot * held[c][partners[k, g]]
                ret[at, :] = pot * held[c][g]
                partial[to, :] = own if k == 0 else partial[to, :] + own
            for eight in range(first, first + count, 8):
                wide = jnp.concatenate(
                    [ret[pl.ds(k * N * BLK + eight + u, N, stride=BLK), :] for u in range(8)], axis=1
                )
                hi, mid = split(wide)
                low = (wide - hi.astype(F32) - mid.astype(F32)).astype(BF16)
                summed = dot(onehots[k], jnp.concatenate([hi, mid, low], axis=0))
                for u in range(min(8, ROWS - eight)):
                    at = pl.ds(eight + u, N, stride=BLK)
                    value = partial[at, :] + summed[:, u * LANES : (u + 1) * LANES]
                    partial[at, :] = value if k == 0 else -MIX * value
        if c == PARTS - 1:
            index_energy = jnp.sum(back[pl.ds(ROWS, PAIRS, stride=BLK), :], axis=0, keepdims=True)
            partial[pl.ds(ROWS, N, stride=BLK), :] = jnp.broadcast_to(index_energy, (N, LANES))
        each_peer(lambda i, c=c: exchange_copy(c, peer(band, i), band).start())
        final[rows_of(band, first, count), :] = partial[rows_of(band, first, count), :]

    def summing_left(i):
        p = peer(band, i)
        if_summing(p, lambda: square_copy(p, p, band).wait_send())

    each_peer(summing_left)
    if_summing(band, lambda: each_peer(lambda i: density_copy(peer(band, i), band).wait_send()))
    for c in range(PARTS):
        each_peer(lambda i, c=c: orbital_copy(c, peer(band, i), band).wait_send())
        for k in range(2):
            each_peer(lambda i, k=k, c=c: pair_copy(k, c, peer(slab, i), slab).wait_send())
            each_peer(lambda i, k=k, c=c: pot_copy(k, c, peer(slab, i), slab).wait_send())

    for c, (first, count) in enumerate(CHUNKS):
        each_peer(lambda i, c=c: exchange_copy(c, peer(band, i), peer(band, i)).wait_recv())
        for r in range(first, min(ROWS, first + count)):
            plane, chunk = divmod(r, 18)
            lanes = slice(chunk * LANES, (chunk + 1) * LANES)
            forces[plane, :, lanes] = (
                local[pl.ds(r, 1), :] * orb[plane, :, lanes] + final[pl.ds(r, N, stride=BLK), :]
            )
    energies = final[pl.ds(ROWS, N, stride=BLK), :]
    energy_out[0, 0] = jnp.sum(energies) * (-1.0 / (2.0 * N * N * NX * NY * NZ))
    for c in range(PARTS):
        each_peer(lambda i, c=c: exchange_copy(c, peer(band, i), band).wait_send())


def solution(mesh):
    dft = constants()
    vmem = pl.BlockSpec(memory_space=pltpu.VMEM)
    smem = pl.BlockSpec(memory_space=pltpu.SMEM)
    hbm = pl.BlockSpec(memory_space=pl.ANY)
    one = pltpu.VMEM((N * BLK, LANES), F32)
    two = pltpu.VMEM((2 * N * BLK, LANES), F32)
    line = pltpu.VMEM((BLK, LANES), F32)
    grid = pltpu.VMEM((48 * 48, LANES), F32)
    sems = lambda n: pltpu.SemaphoreType.DMA((n,))

    def body(orbitals, partners, counts):
        forces, energy = pl.pallas_call(
            kernel,
            out_shape=(
                jax.ShapeDtypeStruct((3, N, NY * NZ), F32),
                jax.ShapeDtypeStruct((1, 1), F32),
            ),
            in_specs=[hbm] * 4,
            out_specs=(vmem, smem),
            scratch_shapes=[
                pltpu.VMEM((3, N, NY * NZ), F32),
                pltpu.SMEM((2, N), jnp.int32),
                pltpu.SMEM((2, N), jnp.int32),
                pltpu.VMEM(dft.shape, BF16),
                one,
                two, two, two, two,
                one, one,
                two,
                line, pltpu.VMEM((N * 8, LANES), F32),
                pltpu.VMEM((8, LANES), F32), line, line,
                grid, grid,
                sems(4),
                sems(PARTS * N), sems(PARTS * N),
                sems(2 * PARTS * N), sems(2 * PARTS * N),
                sems(2 * PARTS * N), sems(2 * PARTS * N),
                sems(PARTS * N), sems(PARTS * N),
                sems(N), sems(N),
                sems(N), sems(N),
                *[pltpu.VMEM((N, count, LANES), F32) for _, count in CHUNKS],
            ],
            compiler_params=pltpu.CompilerParams(
                collective_id=0, has_side_effects=True, vmem_limit_bytes=VMEM_BYTES
            ),
        )(
            orbitals.transpose(1, 0, 2), partners.T, counts.T,
            jnp.asarray(dft),
        )
        return forces.transpose(1, 0, 2), energy.reshape(())

    specs = P("band", "slab", None)
    return jax.shard_map(
        body, mesh=mesh, in_specs=(specs, P(), P()), out_specs=(specs, P()), check_vma=False
    )
```

```python
import functools
import math

import jax
import jax.numpy as jnp
import numpy as np
from jax import lax
from jax.experimental import pallas as pl
from jax.experimental.pallas import tpu as pltpu
from jax.sharding import PartitionSpec as P

NX = 48
NY = 48
NZ = 48
NZP = 96
N = 16
ROWS = 54
BLK = 56
LANES = 128
CHUNKS = ((0, BLK),)
PARTS = len(CHUNKS)
TILES = BLK // 8
PAIRS = 2 * N
SLATER = -((3.0 / math.pi) ** (1.0 / 3.0))
MIX = 0.25
VMEM_BYTES = 56_000_000
SCREENING = 0.25
F32 = jnp.float32
BF16 = jnp.bfloat16
MESH = pl.DeviceIdType.MESH


def split_np(w):
    hi = w.astype(np.float32).astype(jnp.bfloat16)
    lo = (w - hi.astype(np.float64)).astype(np.float32).astype(jnp.bfloat16)
    return hi, lo


def cas(length):
    j = np.arange(length)
    angle = 2.0 * np.pi * ((j[:, None] * j[None, :]) % length) / length
    return (np.cos(angle) + np.sin(angle)) / np.sqrt(length)


def constants():
    h = cas(48)
    order = np.array([3 * p + plane for plane in range(3) for p in range(16)])
    wx = h[:, order]

    def left(w):
        hi, lo = split_np(w)
        return np.concatenate([hi, hi, lo], axis=1)

    small = np.stack([left(wx), left(h), left(wx.T)])
    hz = cas(NZP)[:NZ, :]
    full = np.zeros((384, 8, LANES))
    for y8 in range(8):
        full[y8 * 48 : (y8 + 1) * 48, y8, :NZP] = hz
    full = full.reshape(384, 8 * LANES)
    fwd = np.concatenate(
        [full[0:128, 0:256], full[0:256, 256:512], full[128:384, 512:768], full[256:384, 768:1024]]
    )
    back = full.T
    inv01 = back[0 : 6 * 128, 0:256]
    inv2 = back[5 * 128 : 8 * 128, 256:384]
    small = np.pad(small.reshape(144, 144), ((0, 0), (0, 112)))
    return np.concatenate(
        [*split_np(fwd), *split_np(inv01), np.concatenate(split_np(inv2), axis=1), small]
    )


def split(x):
    hi = x.astype(BF16)
    lo = (x - hi.astype(F32)).astype(BF16)
    return hi, lo


def dot(a, b):
    return jnp.dot(a, b, preferred_element_type=F32)


def dot3(x_hl, w_hi, w_lo, m):
    both = dot(x_hl, w_hi)
    return both[:m] + both[m:] + dot(x_hl[:m], w_lo)


def left3(w3, x):
    hi, lo = split(x)
    return dot(w3, jnp.concatenate([hi, lo, hi], axis=0))


def fill_table(table):
    def wave_sq(index, length):
        signed = jnp.where(index > length // 2, index - length, index).astype(F32)
        wave = 2.0 * math.pi / length * signed
        return wave * wave

    lane = lax.broadcasted_iota(jnp.int32, (48, LANES), 1)
    row = lax.broadcasted_iota(jnp.int32, (48, LANES), 0)
    yz = wave_sq(row, NY) + wave_sq(lane, NZP) + SCREENING * SCREENING

    def step(qx, carry):
        wx = wave_sq(jnp.full((48, LANES), qx, jnp.int32), NX)
        value = jnp.where(lane < NZP, 4.0 * math.pi / (yz + wx), 0.0)
        table[pl.ds(pl.multiple_of(qx * 48, 8), 48), :] = value
        return carry

    lax.fori_loop(0, 48, step, 0)


def convolve(pd, pot, base, work, table, dft):
    rows = 288

    def gather(ref, t):
        tiles = [
            ref[pl.ds(base + plane * 18 + yg * 3 + t, 16, stride=BLK), :]
            for yg in range(6)
            for plane in range(3)
        ]
        return jnp.concatenate(tiles, axis=0)

    def scatter_z(j, value):
        for yg in range(6):
            for half in range(2):
                y = yg * 8 + 2 * j + half
                work[pl.ds(y * 48, 48), :] = value[
                    yg * 48 : (yg + 1) * 48, half * LANES : (half + 1) * LANES
                ]

    def stack(t):
        hi, lo = split(gather(pd, t))
        return jnp.concatenate([hi, lo], axis=0)

    s0 = stack(0)
    scatter_z(0, dot3(s0, dft[0:128], dft[768 : 768 + 128], rows))
    s1 = stack(1)
    s01 = jnp.concatenate([s0, s1], axis=1)
    scatter_z(1, dot3(s01, dft[128:384], dft[768 + 128 : 768 + 384], rows))
    s2 = stack(2)
    s12 = jnp.concatenate([s1, s2], axis=1)
    scatter_z(2, dot3(s12, dft[384:640], dft[768 + 384 : 768 + 640], rows))
    scatter_z(3, dot3(s2, dft[640:768], dft[768 + 640 : 768 + 768], rows))

    def along_x(which):
        w3 = dft[3456 + 48 * which : 3504 + 48 * which, 0:144]

        def step(i, carry):
            start = pl.multiple_of(i * 384, 8)
            block = work[pl.ds(start, 384), :]
            wide = jnp.concatenate([block[48 * u : 48 * (u + 1)] for u in range(8)], axis=1)
            out = left3(w3, wide)
            work[pl.ds(start, 384), :] = jnp.concatenate(
                [out[:, LANES * u : LANES * (u + 1)] for u in range(8)], axis=0
            )
            return carry

        lax.fori_loop(0, 6, step, 0, unroll=6)

    along_x(0)
    wy3 = dft[3504:3552, 0:144]

    def y_step(i, carry):
        qx = i * 8
        wide = jnp.concatenate(
            [work[pl.ds(qx + u, 48, stride=48), :] for u in range(8)], axis=1
        )
        spectrum = left3(wy3, wide)
        k = table[pl.ds(pl.multiple_of(qx * 48, 8), 384), :]
        k = jnp.concatenate([k[48 * u : 48 * (u + 1)] for u in range(8)], axis=1)
        out = left3(wy3, spectrum * k)
        for u in range(8):
            work[pl.ds(qx + u, 48, stride=48), :] = out[:, LANES * u : LANES * (u + 1)]
        return carry

    lax.fori_loop(0, 6, y_step, 0, unroll=6)
    along_x(2)

    def gather_y8(y8):
        tiles = [work[pl.ds((yg * 8 + y8) * 48, 48), :] for yg in range(6)]
        hi, lo = split(jnp.concatenate(tiles, axis=0))
        return jnp.concatenate([hi, lo], axis=0)

    energy = jnp.zeros((16, LANES), F32)

    def scatter_t(t, value, energy):
        for yg in range(6):
            for plane in range(3):
                at = pl.ds(base + plane * 18 + yg * 3 + t, 16, stride=BLK)
                tile = value[(yg * 3 + plane) * 16 : (yg * 3 + plane + 1) * 16]
                pot[at, :] = tile
                energy = energy + tile * pd[at, :]
        return energy

    parts = [gather_y8(y8) for y8 in range(6)]
    first = jnp.concatenate(parts, axis=1)
    out = dot3(first, dft[1536:2304], dft[2304:3072], rows)
    energy = scatter_t(0, out[:, 0:128], energy)
    energy = scatter_t(1, out[:, 128:256], energy)
    second = jnp.concatenate([parts[5], gather_y8(6), gather_y8(7)], axis=1)
    energy = scatter_t(2, dot3(second, dft[3072:3456, 0:128], dft[3072:3456, 128:256], rows), energy)
    total = jnp.sum(energy, axis=0, keepdims=True)
    pot[pl.ds(base + ROWS, 16, stride=BLK), :] = jnp.broadcast_to(total, (16, LANES))


def rows_of(index, first, count):
    return pl.ds(pl.multiple_of(index * BLK + first, 8), count)


def block(index):
    return rows_of(index, 0, BLK)


def kernel(
    orb_hbm, partners_hbm, counts_hbm, dft_hbm,
    forces, energy_out,
    orb, partners, counts, dft,
    src, pairs, tasks, pots, back, partial, final, ret, dens, dens_in, dens_tile, dens_all, local, work, table,
    load_sems, sa, ra, sb, rb, sc, rc, sd, rd, sn, rn, st, rt, *held,
):
    band = lax.axis_index("band")
    slab = lax.axis_index("slab")

    loads = [
        pltpu.make_async_copy(a, b, load_sems.at[i])
        for i, (a, b) in enumerate(
            (
                (orb_hbm, orb), (partners_hbm, partners), (counts_hbm, counts),
                (dft_hbm, dft),
            )
        )
    ]
    for load in loads:
        load.start()

    def peer(me, i):
        j = i - 1
        if me is band:
            h = j // 2
            dz = 4 + lax.rem(h, 2) * -((h + 1) // 2) + (1 - lax.rem(h, 2)) * (h // 2)
            bx = lax.rem(band // 8 + 1 - lax.rem(j, 2), 2)
            return bx * 8 + lax.rem(lax.rem(band, 8) + dz, 8)
        h = j // 4
        dy = jnp.where(h == 0, 2, jnp.where(h == 1, 1, jnp.where(h == 2, 3, 0)))
        low = lax.bitwise_xor(lax.rem(slab, 4), 3 - lax.rem(j, 4))
        return lax.rem(slab // 4 + dy, 4) * 4 + low

    def each_peer(fn):
        def step(i, carry):
            fn(i)
            return carry

        lax.fori_loop(1, N, step, 0)

    barrier = pltpu.get_barrier_semaphore()

    def greet(i):
        pl.semaphore_signal(barrier, inc=1, device_id={"band": peer(band, i)}, device_id_type=MESH)
        pl.semaphore_signal(barrier, inc=1, device_id={"slab": peer(slab, i)}, device_id_type=MESH)

    each_peer(greet)
    loads[0].wait()

    for plane in range(3):
        for chunk in range(18):
            tile = orb[plane, :, chunk * LANES : (chunk + 1) * LANES]
            src[pl.ds(plane * 18 + chunk, N, stride=BLK), :] = tile
    pl.semaphore_wait(barrier, 2 * (N - 1))

    def remote(a, b, send, recv, axis, p):
        return pltpu.make_async_remote_copy(
            src_ref=a, dst_ref=b, send_sem=send, recv_sem=recv,
            device_id={axis: p}, device_id_type=MESH,
        )

    def orbital_copy(c, p, at):
        first, count = CHUNKS[c]
        return remote(
            src.at[rows_of(p, first, count)], held[c].at[at],
            sa.at[c * N + p], ra.at[c * N + at], "band", p,
        )

    def tile_of(index):
        return pl.ds(pl.multiple_of(index * 8, 8), 8)

    def square_copy(p, tile, at):
        return remote(dens.at[tile_of(tile)], dens_in.at[tile_of(at)], sn.at[p], rn.at[at], "band", p)

    def density_copy(p, tile):
        return remote(dens_tile, dens_all.at[tile_of(tile)], st.at[p], rt.at[tile], "band", p)

    def if_summing(index, fn):
        pl.when(index < TILES)(fn)

    def pair_copy(k, c, p, at):
        first, count = CHUNKS[c]
        sem = (k * PARTS + c) * N
        return remote(
            pairs.at[rows_of(k * N + p, first, count)], tasks.at[rows_of(k * N + at, first, count)],
            sb.at[sem + p], rb.at[sem + at], "slab", p,
        )

    def pot_copy(k, c, p, at):
        first, count = CHUNKS[c]
        sem = (k * PARTS + c) * N
        return remote(
            pots.at[rows_of(k * N + p, first, count)], back.at[rows_of(k * N + at, first, count)],
            sc.at[sem + p], rc.at[sem + at], "slab", p,
        )

    def exchange_copy(c, p, at):
        first, count = CHUNKS[c]
        return remote(
            partial.at[rows_of(p, first, count)], final.at[rows_of(at, first, count)],
            sd.at[c * N + p], rd.at[c * N + at], "band", p,
        )

    for c in range(PARTS):
        each_peer(lambda i, c=c: orbital_copy(c, peer(band, i), band).start())
    for c, (first, count) in enumerate(CHUNKS):
        held[c][band] = src[rows_of(band, first, count), :]
    for plane in range(3):
        for chunk in range(18):
            tile = orb[plane, :, chunk * LANES : (chunk + 1) * LANES]
            dens[pl.ds(plane * 18 + chunk, 1), :] = jnp.sum(tile * tile, axis=0, keepdims=True)

    def to_summing(i):
        p = peer(band, i)
        if_summing(p, lambda: square_copy(p, p, band).start())

    each_peer(to_summing)

    @pl.when(band < TILES)
    def _():
        dens_in[tile_of(band), :] = dens[tile_of(band), :]

    fill_table(table)
    loads[1].wait()
    loads[2].wait()

    for c, (first, count) in enumerate(CHUNKS):
        each_peer(lambda i, c=c: orbital_copy(c, peer(band, i), peer(band, i)).wait_recv())
        for g in range(N):
            mine = held[c][g]
            for k in range(2):
                active = jnp.where(band < counts[k, g], 1.0, 0.0).astype(F32)
                product = mine * held[c][partners[k, g]] * active
                pairs[pl.ds((k * N + g) * BLK + first, count), :] = product
        for k in range(2):
            if k == 0:
                each_peer(lambda i, k=k, c=c: pair_copy(k, c, peer(slab, i), slab).start())
            at = rows_of(k * N + slab, first, count)
            tasks[at, :] = pairs[at, :]

    @pl.when(band < TILES)
    def _():
        each_peer(lambda i: square_copy(peer(band, i), band, peer(band, i)).wait_recv())
        summed = dens_in[0:8, :]
        for b in range(1, N):
            summed = summed + dens_in[b * 8 : (b + 1) * 8, :]
        dens_tile[...] = summed
        dens_all[tile_of(band), :] = summed
        each_peer(lambda i: density_copy(peer(band, i), band).start())

    for load in loads[3:]:
        load.wait()

    for k in range(2):
        for c in range(PARTS):
            def pair_in(i, k=k, c=c):
                p = peer(slab, i)
                pair_copy(k, c, p, p).wait_recv()
                if k == 0:
                    pair_copy(1, c, p, slab).start()

            each_peer(pair_in)
        convolve(tasks, pots, k * N * BLK, work, table, dft)
        for c in range(PARTS):
            each_peer(lambda i, k=k, c=c: pot_copy(k, c, peer(slab, i), slab).start())
        back[block(k * N + slab), :] = pots[block(k * N + slab), :]

    def from_summing(i):
        p = peer(band, i)
        if_summing(p, lambda: density_copy(p, p).wait_recv())

    each_peer(from_summing)
    total = dens_all[...]
    total = total * (2.0 / (N * N))
    safe = jnp.maximum(total, 1e-37)
    root = jnp.exp(jnp.log(safe) * (1.0 / 3.0))
    root = root * (2.0 + safe / (root * root * root)) * (1.0 / 3.0)
    local[...] = SLATER * jnp.where(total > 0.0, root, 0.0)

    row = lax.broadcasted_iota(jnp.int32, (N, N), 0)
    col = lax.broadcasted_iota(jnp.int32, (N, N), 1)
    onehots = []
    for k in range(2):
        names = jnp.full((N, N), -1, jnp.int32)
        for g in range(N):
            names = jnp.where(col == g, partners[k, g], names)
        onehot = jnp.where(names == row, 1.0, 0.0).astype(BF16)
        onehots.append(jnp.concatenate([onehot, onehot, onehot], axis=1))

    for c, (first, count) in enumerate(CHUNKS):
        for k in range(2):
            each_peer(lambda i, k=k, c=c: pot_copy(k, c, peer(slab, i), peer(slab, i)).wait_recv())
            for g in range(N):
                at = pl.ds((k * N + g) * BLK + first, count)
                to = pl.ds(g * BLK + first, count)
                pot = back[at, :]
                own = pot * held[c][partners[k, g]]
                ret[at, :] = pot * held[c][g]
                partial[to, :] = own if k == 0 else partial[to, :] + own
            for eight in range(first, first + count, 8):
                wide = jnp.concatenate(
                    [ret[pl.ds(k * N * BLK + eight + u, N, stride=BLK), :] for u in range(8)], axis=1
                )
                hi, mid = split(wide)
                low = (wide - hi.astype(F32) - mid.astype(F32)).astype(BF16)
                summed = dot(onehots[k], jnp.concatenate([hi, mid, low], axis=0))
                for u in range(min(8, ROWS - eight)):
                    at = pl.ds(eight + u, N, stride=BLK)
                    value = partial[at, :] + summed[:, u * LANES : (u + 1) * LANES]
                    partial[at, :] = value if k == 0 else -MIX * value
        if c == PARTS - 1:
            index_energy = jnp.sum(back[pl.ds(ROWS, PAIRS, stride=BLK), :], axis=0, keepdims=True)
            partial[pl.ds(ROWS, N, stride=BLK), :] = jnp.broadcast_to(index_energy, (N, LANES))
        each_peer(lambda i, c=c: exchange_copy(c, peer(band, i), band).start())
        final[rows_of(band, first, count), :] = partial[rows_of(band, first, count), :]

    def summing_left(i):
        p = peer(band, i)
        if_summing(p, lambda: square_copy(p, p, band).wait_send())

    each_peer(summing_left)
    if_summing(band, lambda: each_peer(lambda i: density_copy(peer(band, i), band).wait_send()))
    for c in range(PARTS):
        each_peer(lambda i, c=c: orbital_copy(c, peer(band, i), band).wait_send())
        for k in range(2):
            each_peer(lambda i, k=k, c=c: pair_copy(k, c, peer(slab, i), slab).wait_send())
            each_peer(lambda i, k=k, c=c: pot_copy(k, c, peer(slab, i), slab).wait_send())

    for c, (first, count) in enumerate(CHUNKS):
        each_peer(lambda i, c=c: exchange_copy(c, peer(band, i), peer(band, i)).wait_recv())
        for r in range(first, min(ROWS, first + count)):
            plane, chunk = divmod(r, 18)
            lanes = slice(chunk * LANES, (chunk + 1) * LANES)
            forces[plane, :, lanes] = (
                local[pl.ds(r, 1), :] * orb[plane, :, lanes] + final[pl.ds(r, N, stride=BLK), :]
            )
    energies = final[pl.ds(ROWS, N, stride=BLK), :]
    energy_out[0, 0] = jnp.sum(energies) * (-1.0 / (2.0 * N * N * NX * NY * NZ))
    for c in range(PARTS):
        each_peer(lambda i, c=c: exchange_copy(c, peer(band, i), band).wait_send())


def solution(mesh):
    dft = constants()
    vmem = pl.BlockSpec(memory_space=pltpu.VMEM)
    smem = pl.BlockSpec(memory_space=pltpu.SMEM)
    hbm = pl.BlockSpec(memory_space=pl.ANY)
    one = pltpu.VMEM((N * BLK, LANES), F32)
    two = pltpu.VMEM((2 * N * BLK, LANES), F32)
    line = pltpu.VMEM((BLK, LANES), F32)
    grid = pltpu.VMEM((48 * 48, LANES), F32)
    sems = lambda n: pltpu.SemaphoreType.DMA((n,))

    def body(orbitals, partners, counts):
        forces, energy = pl.pallas_call(
            kernel,
            out_shape=(
                jax.ShapeDtypeStruct((3, N, NY * NZ), F32),
                jax.ShapeDtypeStruct((1, 1), F32),
            ),
            in_specs=[hbm] * 4,
            out_specs=(vmem, smem),
            scratch_shapes=[
                pltpu.VMEM((3, N, NY * NZ), F32),
                pltpu.SMEM((2, N), jnp.int32),
                pltpu.SMEM((2, N), jnp.int32),
                pltpu.VMEM(dft.shape, BF16),
                one,
                two, two, two, two,
                one, one,
                two,
                line, pltpu.VMEM((N * 8, LANES), F32),
                pltpu.VMEM((8, LANES), F32), line, line,
                grid, grid,
                sems(4),
                sems(PARTS * N), sems(PARTS * N),
                sems(2 * PARTS * N), sems(2 * PARTS * N),
                sems(2 * PARTS * N), sems(2 * PARTS * N),
                sems(PARTS * N), sems(PARTS * N),
                sems(N), sems(N),
                sems(N), sems(N),
                *[pltpu.VMEM((N, count, LANES), F32) for _, count in CHUNKS],
            ],
            compiler_params=pltpu.CompilerParams(
                collective_id=0, has_side_effects=True, vmem_limit_bytes=VMEM_BYTES
            ),
        )(
            orbitals.transpose(1, 0, 2), partners.T, counts.T,
            jnp.asarray(dft),
        )
        return forces.transpose(1, 0, 2), energy.reshape(())

    specs = P("band", "slab", None)
    return jax.shard_map(
        body, mesh=mesh, in_specs=(specs, P(), P()), out_specs=(specs, P()), check_vma=False
    )
```
